32 devices in a mesh: dp: 4 (over x, core), seq: 8 (over z, y).
Axes of the slice: x: 2, y: 2, z: 4, core: 2. Of those that a mesh axis runs over, the one named last changes fastest.
Arguments:
- tokens: bfloat16 [4096, 1152], P(('dp', 'seq')), may hold values from -6 to 6
- route: int32 [4096, 1], P(('dp', 'seq')), may hold values from 0 to 3; in each aligned block of 128 rows (0 to 127, 128 to 255, ...) at most 40 rows name the same one
- cotangent: bfloat16 [4096, 1152], P(('dp', 'seq')), may hold values from -6 to 6
- gain_mix: bfloat16 [1152], P(('dp', 'seq')), may hold values from 0.5 to 1.5
- w_in: bfloat16 [1152, 4608], P(('dp', 'seq')), may hold values from -0.1875 to 0.1875
- conv_w: bfloat16 [2304, 4], P(('dp', 'seq')), may hold values from -3 to 3
- w_x: bfloat16 [2304, 104], P(('dp', 'seq')), may hold values from -0.125 to 0.125
- w_dt: bfloat16 [2304, 72], P(('dp', 'seq')), may hold values from -0.75 to 0.75
- dt_bias: bfloat16 [2304], P(('dp', 'seq')), may hold values from -5 to -4.1875
- a_log: bfloat16 [2304, 16], P(('dp', 'seq')), as said below
- d_skip: bfloat16 [2304], P(('dp', 'seq')), may hold values from 0.5 to 1.5
- w_out: bfloat16 [2304, 1152], P(('dp', 'seq')), may hold values from -0.25 to 0.25
- gain_moe: bfloat16 [1152], P(('dp', 'seq')), may hold values from 0.5 to 1.5
- w_up: bfloat16 [4, 3072, 1152], P('dp', 'seq'), may hold values from -0.1875 to 0.1875
- w_down: bfloat16 [4, 3072, 1152], P('dp', 'seq'), may hold values from -0.21875 to 0.21875
Outputs:
- result: bfloat16 [4096, 1152], P(('dp', 'seq'))
- grad_tokens: float32 [4096, 1152], P(('dp', 'seq'))
- grad_gain_mix: float32 [1152], P(('dp', 'seq'))
- grad_w_in: float32 [1152, 4608], P(('dp', 'seq'))
- grad_conv_w: float32 [2304, 4], P(('dp', 'seq'))
- grad_w_x: float32 [2304, 104], P(('dp', 'seq'))
- grad_w_dt: float32 [2304, 72], P(('dp', 'seq'))
- grad_dt_bias: float32 [2304], P(('dp', 'seq'))
- grad_a_log: float32 [2304, 16], P(('dp', 'seq'))
- grad_d_skip: float32 [2304], P(('dp', 'seq'))
- grad_w_out: float32 [2304, 1152], P(('dp', 'seq'))
- grad_gain_moe: float32 [1152], P(('dp', 'seq'))
- grad_w_up: float32 [4, 3072, 1152], P('dp', 'seq')
- grad_w_down: float32 [4, 3072, 1152], P('dp', 'seq')
The draws below stay inside these ranges and needn't reach their ends.
Inputs may be any that keep to these rules, and one draw needn't show every extreme that they name: `route`: in each aligned block of 128 tokens no expert is named by more than 40 tokens, a bound that some block reaches. `a_log`: finite values.
All inputs are finite; a program needn't handle non-finite values.
Results may differ from the reference program's by a relative error of at most 0.014.
Values may be sent and summed in bfloat16 or wider, within the bound.
A program may use at most 256 MiB of HBM per device.

```python
import math
import jax
import jax.numpy as jnp
import numpy as np
from jax import lax

D = 1152
DI = 2304
NS = 16
RANK = 72
E = 4
FF = 3072
TOK_DEV = 128
CAP = 40
LEN = 1024
TOKENS = 4096
N_DP = 4


def draw_a_log(key, part):
    key_kind = jax.random.fold_in(key, 11)
    key_scale = jax.random.fold_in(key, 12)
    share = 0.5
    slow_mask = jax.random.uniform(key_kind, (DI, 1), dtype=jnp.float32) < share
    factor = jnp.exp(jax.random.uniform(key_scale, (DI, NS), dtype=jnp.float32, minval=-0.7, maxval=0.7))
    slow_rate = 60.0 / LEN
    rate_values = jnp.where(slow_mask, slow_rate, 2.5) * factor
    return jnp.log(rate_values).astype(jnp.bfloat16)


def shard_levels(key, shape, cuts, smallest, top_value):
    level = 1.0
    for axis_at, shards_of in cuts:
        steps = jax.random.uniform(jax.random.fold_in(jax.random.fold_in(key, 6), axis_at), (shards_of,), jnp.float32, smallest / len(cuts), top_value / len(cuts))
        level = level * jnp.repeat(jnp.exp(steps), shape[axis_at] // shards_of).reshape((-1,) + (1,) * (len(shape) - 1 - axis_at))
    return level


def deal_out(own_key, own, number, rows, number_of, top, reach, lean):
    sequence = jax.random.permutation(own_key, number_of)
    packed, usual = shares(number_of, rows * top, reach, lean, True), shares(number_of, rows * top, reach, lean, False)
    places = jnp.arange(number_of)

    def named(sizes, turn):
        used = int((sizes > 0).sum())
        fixed = max(1, used // 4)
        passed = fixed + (places - fixed + turn * (used - fixed)) % max(1, number_of - fixed)
        return jnp.zeros((number_of,), jnp.int32).at[sequence[jnp.where(places < fixed, places, passed)]].set(jnp.asarray(sizes, jnp.int32))

    sizes = jnp.where(number % 4 == 0, named(packed, number // 4), named(usual, number - number // 4 - 1))
    mixed = jax.random.permutation(jax.random.fold_in(own, 3), number_of)
    giver, receiver = mixed[0:number_of // 2 * 2:2], mixed[1:number_of // 2 * 2:2]
    margin = jnp.minimum(sizes[giver] - 1, reach - sizes[receiver]) // 2
    margin = jnp.where((giver == sequence[0]) | (receiver == sequence[0]) | (sizes[receiver] == 0), 0, jnp.maximum(margin, 0))
    passed = jax.random.randint(jax.random.fold_in(own, 4), (number_of // 2,), 0, 1 << 20) % (margin + 1)
    sizes = sizes.at[giver].add(-passed).at[receiver].add(passed)
    members = jnp.searchsorted(jnp.cumsum(sizes), jnp.arange(rows * top), side="right").astype(jnp.int32)
    table = members.reshape(top, rows).T
    table = table[jax.random.permutation(jax.random.fold_in(own, 1), rows)]
    turn = jax.random.randint(jax.random.fold_in(own, 2), (rows, 1), 0, top)
    return jnp.take_along_axis(table, (jnp.arange(top)[None, :] + turn) % top, axis=1)


def shares(number_of, total, limit, lean, full):
    portions = [(1 << 20) // math.isqrt(rank ** lean) + 1 for rank in range(1, number_of + 1)]
    largest = limit if full else min(limit, max(-(-total // number_of), total * portions[0] // sum(portions)))
    least = 1 if total - largest >= number_of - 1 else 0
    given, rest = [largest] + [least] * (number_of - 1), total - largest - least * (number_of - 1)
    while rest > 0:
        free = [i for i in range(1, number_of) if given[i] < largest] or [i for i in range(1, number_of) if given[i] < limit]
        pool, remaining = sum([portions[i] for i in free]), rest
        for i in free:
            more = min(limit - given[i], max(1, remaining * portions[i] // pool), rest)
            given[i] = given[i] + more
            rest = rest - more
    return np.array(given)


def normal_values(rng, extent, spread, most, split=(), kind=jnp.bfloat16):
    array = jax.random.normal(rng, extent, jnp.float32) * spread
    if len(split) > 0:
        array = shard_levels(rng, extent, split, -0.22, 0.18) * array
    return jnp.clip(array, min=-most, max=most).astype(kind)


def setup_inputs(seed: int = 0) -> dict:
    streams_of = jax.random.split(jax.random.key(seed), 16)
    tokens = normal_values(streams_of[0], (TOKENS, D), 1.0, 6.0, ((0, 32),))
    route_keys = jax.random.split(jax.random.fold_in(streams_of[1], 1), TOKENS // TOK_DEV)
    route_turns = jax.random.permutation(jax.random.fold_in(streams_of[1], 3), TOKENS // TOK_DEV)
    route = jax.vmap(lambda own, number: deal_out(jax.random.fold_in(streams_of[1], 2), own, number, TOK_DEV, E, 1, CAP, 1))(route_keys, route_turns).reshape((TOKENS, 1))
    cotangent = normal_values(streams_of[2], (TOKENS, D), 1.0, 6.0, ((0, 32),))
    gain_mix = jnp.clip(1.0 + 0.1 * jax.random.normal(streams_of[3], (D,), jnp.float32), 0.5, 1.5).astype(jnp.bfloat16)
    w_in = normal_values(streams_of[4], (D, 2 * DI), D ** -0.5, 0.1875, ((0, 32),))
    conv_w = normal_values(streams_of[5], (DI, 4), 4 ** -0.5, 3.0, ((0, 32),))
    w_x = normal_values(streams_of[6], (DI, RANK + 2 * NS), DI ** -0.5, 0.125, ((0, 32),))
    w_dt = normal_values(streams_of[7], (DI, RANK), RANK ** -0.5, 0.75, ((0, 32),))
    dt_bias = jnp.clip(-5.0 + 0.8125 * jax.random.uniform(streams_of[8], (DI,), jnp.float32) ** shard_levels(streams_of[8], (DI,), ((0, 32),), -0.2, 0.2), -5.0, -4.1875).astype(jnp.bfloat16)
    a_log = draw_a_log(jax.random.fold_in(streams_of[15], 71), 0)
    d_skip = jnp.clip(0.5 + 1.0 * jax.random.uniform(streams_of[10], (DI,), jnp.float32) ** shard_levels(streams_of[10], (DI,), ((0, 32),), -0.2, 0.2), 0.5, 1.5).astype(jnp.bfloat16)
    w_out = normal_values(streams_of[11], (DI, D), (DI // 4) ** -0.5, 0.25, ((0, 32),))
    gain_moe = jnp.clip(1.0 + 0.1 * jax.random.normal(streams_of[12], (D,), jnp.float32), 0.5, 1.5).astype(jnp.bfloat16)
    w_up = normal_values(streams_of[13], (E, FF, D), D ** -0.5, 0.1875, ((0, 4), (1, 8)))
    w_down = normal_values(streams_of[14], (E, FF, D), (FF // 4) ** -0.5, 0.21875, ((0, 4), (1, 8)))
    return dict(tokens=tokens, route=route, cotangent=cotangent, gain_mix=gain_mix, w_in=w_in, conv_w=conv_w, w_x=w_x, w_dt=w_dt, dt_bias=dt_bias, a_log=a_log, d_skip=d_skip, w_out=w_out, gain_moe=gain_moe, w_up=w_up, w_down=w_down)


eps = 1e-05

@jax.custom_vjp
def low(v):
    return lax.optimization_barrier(v.astype(jnp.bfloat16)).astype(jnp.float32)

@jax.custom_vjp
def low_back(v):
    return v

def low_keep(v):
    return (low(v), None)

def low_pass(kept, grad):
    return (grad,)

def back_keep(v):
    return (v, None)

def back_low(kept, grad):
    return (low(grad),)
low.defvjp(low_keep, low_pass)
low_back.defvjp(back_keep, back_low)

def matmul(left, right):
    return jnp.dot(left, right, precision=lax.Precision.HIGHEST, preferred_element_type=jnp.float32)

def rms_norm(values, gain_vec):
    return values * lax.rsqrt(lax.optimization_barrier(jnp.mean(values * values, axis=-1, keepdims=True)) + eps) * gain_vec

def conv_silu(x_part, tail_prev, conv_w):
    padded = jnp.concatenate([tail_prev, x_part], axis=0)
    length = x_part.shape[0]
    mixed_taps = padded[0:length] * conv_w[:, 0] + padded[1:length + 1] * conv_w[:, 1]
    mixed_taps = mixed_taps + padded[2:length + 2] * conv_w[:, 2] + padded[3:length + 3] * conv_w[:, 3]
    return jax.nn.silu(mixed_taps)

def combine_pairs(earlier, later_map):
    return (earlier[0] * later_map[0], later_map[0] * earlier[1] + later_map[1])

def ssm_scan(delta, bmat, cmat, u_vals, a_neg):
    length = delta.shape[0]
    block_rows = 64
    block_count = length // block_rows

    def one_block(carry_state, row_values):
        delta_b, b_part, c_part, u_part = row_values
        decay_step = jnp.exp(delta_b[:, None, :] * a_neg[None])
        drive_step = (delta_b * u_part)[:, None, :] * b_part[:, :, None]
        cum_decay, cum_drive = lax.associative_scan(combine_pairs, (decay_step, drive_step), axis=0)
        states = cum_decay * carry_state[None] + cum_drive
        outputs = lax.optimization_barrier(jnp.sum(states * c_part[:, :, None], axis=1))
        return (states[-1], outputs)
    shaped = tuple((v.reshape(block_count, block_rows, v.shape[1]) for v in (delta, bmat, cmat, u_vals)))
    start_state = jnp.zeros((NS, DI), jnp.float32)
    final_state, outputs = lax.scan(jax.checkpoint(one_block), start_state, shaped)
    return outputs.reshape(length, DI)

def one_sequence(params, values, choose):
    gain_mix, w_in, conv_w, w_x, w_dt, dt_bias, a_log, d_skip, w_out, gain_moe, w_up, w_down = params
    normed = rms_norm(values, gain_mix)
    projected = low_back(matmul(low(normed), w_in))
    x_part = projected[:, :DI]
    z_part = projected[:, DI:]
    u_vals = conv_silu(x_part, jnp.zeros((3, DI), jnp.float32), conv_w)
    small = low_back(matmul(low(u_vals), w_x))
    dt_pre = low_back(matmul(low(small[:, :RANK]), w_dt.T))
    delta = jax.nn.softplus(dt_pre + dt_bias)
    a_neg = -jnp.exp(a_log).T
    ssm_out = ssm_scan(delta, small[:, RANK:RANK + NS], small[:, RANK + NS:], u_vals, a_neg)
    gated = (ssm_out + d_skip * u_vals) * jax.nn.silu(z_part)
    mixer_out = low_back(matmul(low(gated), w_out))
    resid = values + mixer_out
    moe_in = low_back(low(rms_norm(resid, gain_moe)))
    onehot = (choose[:, None] == jnp.arange(E, dtype=jnp.int32)[None, :]).astype(jnp.int32)
    blocks = onehot.reshape(LEN // TOK_DEV, TOK_DEV, E)
    slot_index = lax.optimization_barrier(jnp.sum((jnp.cumsum(blocks, axis=1) - 1) * blocks, axis=2)).reshape(LEN).astype(jnp.int32)
    place = jnp.arange(LEN, dtype=jnp.int32) // TOK_DEV * CAP + slot_index
    buffer = jnp.zeros((E, LEN // TOK_DEV * CAP, D), jnp.float32).at[choose, place].set(moe_in)
    pre_act = low_back(jnp.einsum('ecd,efd->ecf', buffer, w_up, precision=lax.Precision.HIGHEST))
    hidden = low(jax.nn.gelu(pre_act, approximate=False))
    expert_out = low_back(low(jnp.einsum('ecf,efd->ecd', hidden, w_down, precision=lax.Precision.HIGHEST)))
    return resid + expert_out[choose, place]

def reference(tokens, route, cotangent, gain_mix, w_in, conv_w, w_x, w_dt, dt_bias, a_log, d_skip, w_out, gain_moe, w_up, w_down):
    params = tuple((p.astype(jnp.float32) for p in (gain_mix, w_in, conv_w, w_x, w_dt, dt_bias, a_log, d_skip, w_out, gain_moe, w_up, w_down)))
    values = tokens.astype(jnp.float32).reshape(N_DP, LEN, D)
    routes = route.reshape(N_DP, LEN).astype(jnp.int32)

    def forward(params, values):

        def seq_step(carry_value, seq_pair):
            return (carry_value, jax.checkpoint(one_sequence)(params, seq_pair[0], seq_pair[1]))
        _, all_outputs = lax.scan(seq_step, jnp.zeros((), jnp.float32), (values, routes))
        return all_outputs
    all_outputs, pullback = jax.vjp(forward, params, values)
    grad_params, grad_values = pullback(cotangent.astype(jnp.float32).reshape(N_DP, LEN, D))
    return (all_outputs.reshape(TOKENS, D).astype(jnp.bfloat16), grad_values.reshape(TOKENS, D), grad_params[0], grad_params[1], grad_params[2], grad_params[3], grad_params[4], grad_params[5], grad_params[6], grad_params[7], grad_params[8], grad_params[9], grad_params[10], grad_params[11])
```

```python
from functools import partial

import jax
import jax.numpy as jnp
from jax import lax
from jax.experimental import pallas as pl
from jax.experimental.pallas import tpu as pltpu
from jax.sharding import PartitionSpec as P

NS = 16
LN2 = 0.6931471805599453
LOG2E = 1.4426950408889634
eps = 1e-05
f32 = jnp.float32
bf16 = jnp.bfloat16

NN = (((1,), (0,)), ((), ()))
NT = (((1,), (1,)), ((), ()))
TN = (((0,), (0,)), ((), ()))


def mm(left, right, dims=NN):
    return lax.dot_general(left, right, dims, preferred_element_type=f32)


def up128(count):
    return -(-count // 128) * 128


def rms_norm(values, gain_vec):
    return values * lax.rsqrt(jnp.mean(values * values, axis=-1, keepdims=True) + eps) * gain_vec


def sigmoid(v):
    return 1.0 / (1.0 + jnp.exp(-v))


def softplus(v):
    return jnp.maximum(v, 0.0) + jnp.log1p(jnp.exp(-jnp.abs(v)))


def tree_step(first, second, by):
    row = lax.broadcasted_iota(jnp.int32, first.shape, 0)
    clear = (row & by) == 0
    return jnp.where(clear, first, second) + pltpu.roll(jnp.where(clear, second, first), by, 0)


def tree_push(stack, value, falling=False):
    level = 1
    while stack and stack[-1][0] == level:
        other = stack.pop()[1]
        value = tree_step(value, other, level) if falling else tree_step(other, value, level)
        level *= 2
    stack.append((level, value))


def in_kernel(xg, w, cw, wx, x_out, z_out, conv_out, small_out, buf):
    rows, cp = x_out.shape

    @pl.when(pl.program_id(0) == 0)
    def _():
        buf[0:8, :] = jnp.zeros((8, cp), f32)

    @pl.when(pl.program_id(0) > 0)
    def _():
        buf[0:8, :] = buf[rows : rows + 8, :]

    prod = mm(xg[...], w[...])
    x_part = prod[:, :cp]
    x_out[...] = x_part
    z_out[...] = prod[:, cp:]
    buf[8 : 8 + rows, :] = x_part
    conv = x_part * cw[3:4, :]
    for k in range(3):
        conv = conv + buf[5 + k : 5 + k + rows, :] * cw[k : k + 1, :]
    conv_out[...] = conv
    small_out[...] = mm((conv * sigmoid(conv)).astype(bf16), wx[...])


def scan_kernel(
    small, bct, wdtt, vecs, a2, conv, z, wout, dtp_out, h_out, ssm_out, gated_out, part_out,
    delta_s, du_s, state,
):
    rows, cp = conv.shape

    @pl.when(pl.program_id(0) == 0)
    def _():
        state[...] = jnp.zeros_like(state)

    dtp = mm(small[...].astype(bf16), wdtt[...]) + vecs[0:1, :]
    dtp_out[...] = dtp
    delta = softplus(dtp)
    cv = conv[...]
    u = cv * sigmoid(cv)
    delta_s[...] = delta
    du_s[...] = delta * u

    def group(g, h):
        base = pl.multiple_of(g * 8, 8)
        bc = bct[g]
        stack = []
        for t in range(8):
            d = jnp.broadcast_to(delta_s[pl.ds(base + t, 1), :], (NS, cp))
            du = jnp.broadcast_to(du_s[pl.ds(base + t, 1), :], (NS, cp))
            h = jnp.exp2(d * a2[...]) * h + du * bc[:NS, t : t + 1]
            h_out[base + t] = h
            prod = h * bc[NS:, t : t + 1]
            tree_push(stack, prod[:8] + prod[8:])
        ssm_out[pl.ds(base, 8), :] = stack[0][1]
        return h

    state[...] = lax.fori_loop(0, rows // 8, group, state[...])
    zv = z[...]
    gated = (ssm_out[...] + vecs[1:2, :] * u) * (zv * sigmoid(zv))
    low = gated.astype(bf16)
    gated_out[...] = low
    part_out[...] = mm(low, wout[...]).astype(part_out.dtype)


def back_kernel(
    gml, wout, gated, conv, z, ssm, dtp, hs, hlast, bct, small, wdt, vecs, a2,
    rank_out, gbct_out, gu_out, gz_out, gwout, gwdt, ga, gvecs,
    delta_s, du_s, gs_s, r1_s, r2_s, lam_s,
):
    rows, cp = conv.shape
    step = pl.program_id(0)
    last = pl.num_programs(0) - 1

    @pl.when(step == 0)
    def _():
        lam_s[...] = jnp.zeros_like(lam_s)
        gwout[...] = jnp.zeros_like(gwout)
        gwdt[...] = jnp.zeros_like(gwdt)
        ga[...] = jnp.zeros_like(ga)
        gvecs[...] = jnp.zeros_like(gvecs)

    grad_mixed = gml[...]
    gg = mm(grad_mixed, wout[...], NT)
    gwout[...] += mm(gated[...], grad_mixed, TN)
    zv = z[...]
    sz = sigmoid(zv)
    cv = conv[...]
    u = cv * sigmoid(cv)
    skip = vecs[1:2, :]
    gz_out[...] = (gg * (ssm[...] + skip * u) * (sz * (1.0 + zv * (1.0 - sz)))).astype(bf16)
    gs = gg * (zv * sz)
    delta = softplus(dtp[...])
    gs_s[...] = gs
    delta_s[...] = delta
    du_s[...] = delta * u
    lane = lax.broadcasted_iota(jnp.int32, (NS, 128), 1)
    keep_first = jnp.where(step == last, 0.0, 1.0)
    tiles = cp // 128

    def lane_fold(v):
        total = v[:, :128]
        for i in range(1, tiles):
            total = total + v[:, i * 128 : (i + 1) * 128]
        return jnp.sum(total, axis=1, keepdims=True)

    def group(k, carry):
        lamd, acc = carry
        g = rows // 8 - 1 - k
        base = pl.multiple_of(g * 8, 8)
        bc = bct[g]
        stack1, stack2 = [], []
        gb = jnp.zeros((NS, 128), f32)
        gc = jnp.zeros((NS, 128), f32)
        h = hs[base + 7]
        ones, twos = {}, {}
        for t in range(7, -1, -1):
            d = jnp.broadcast_to(delta_s[pl.ds(base + t, 1), :], (NS, cp))
            du = jnp.broadcast_to(du_s[pl.ds(base + t, 1), :], (NS, cp))
            g_s = jnp.broadcast_to(gs_s[pl.ds(base + t, 1), :], (NS, cp))
            if t > 0:
                before = hs[base + t - 1]
            else:
                inside = hs[jnp.maximum(base - 1, 0)]
                before = jnp.where(g == 0, hlast[0] * keep_first, inside)
            lam = lamd + g_s * bc[NS:, t : t + 1]
            gc = jnp.where(lane == t, lane_fold(g_s * h), gc)
            gb = jnp.where(lane == t, lane_fold(lam * du), gb)
            lamd = jnp.exp2(d * a2[...]) * lam
            w = lamd * before
            acc = acc + w * d
            wa = w * a2[...]
            lb = lam * bc[:NS, t : t + 1]
            tree_push(stack1, wa[:8] + wa[8:], True)
            tree_push(stack2, lb[:8] + lb[8:], True)
            h = before
        r1_s[pl.ds(base, 8), :] = stack1[0][1]
        r2_s[pl.ds(base, 8), :] = stack2[0][1]
        gbct_out[g, :NS, :] = gb[:, :8]
        gbct_out[g, NS:, :] = gc[:, :8]
        return lamd, acc

    lamd, acc = lax.fori_loop(0, rows // 8, group, (lam_s[...], jnp.zeros((NS, cp), f32)))
    lam_s[...] = lamd
    ga[...] += acc
    r2 = r2_s[...]
    gu_out[...] = skip * gs + delta * r2
    gdelta = r1_s[...] * LN2 + u * r2
    gdtp = gdelta * sigmoid(dtp[...])
    gvecs[0:1, :] += jnp.sum(gdtp, axis=0, keepdims=True)
    gvecs[1:2, :] += jnp.sum(gs * u, axis=0, keepdims=True)
    low = gdtp.astype(bf16)
    gwdt[...] += mm(low, small[...].astype(bf16), TN)
    rank_out[...] = mm(low, wdt[...])


def out_kernel(
    gsmall, wx, conv, x, gu, gz, xg, w, cw, part_out, gwx, gw, gcw, buf
):
    rows, cp = conv.shape

    @pl.when(pl.program_id(0) == 0)
    def _():
        buf[rows : rows + 8, :] = jnp.zeros((8, cp), f32)
        gwx[...] = jnp.zeros_like(gwx)
        gw[...] = jnp.zeros_like(gw)
        gcw[...] = jnp.zeros_like(gcw)

    @pl.when(pl.program_id(0) > 0)
    def _():
        buf[rows : rows + 8, :] = buf[0:8, :]

    gsl = gsmall[...].astype(bf16)
    cv = conv[...]
    s = sigmoid(cv)
    gwx[...] += mm((cv * s).astype(bf16), gsl, TN)
    gconv = (gu[...] + mm(gsl, wx[...], NT)) * (s * (1.0 + cv * (1.0 - s)))
    buf[0:rows, :] = gconv
    xv = x[...]
    gx = gconv * cw[3:4, :]
    gcw[3:4, :] += jnp.sum(gconv * xv, axis=0, keepdims=True)
    for k in range(3):
        moved = buf[3 - k : 3 - k + rows, :]
        gx = gx + moved * cw[k : k + 1, :]
        gcw[k : k + 1, :] += jnp.sum(moved * xv, axis=0, keepdims=True)
    gp = jnp.concatenate([gx.astype(bf16), gz[...]], axis=1)
    part_out[...] = mm(gp, w[...], NT).astype(part_out.dtype)
    gw[...] += mm(xg[...], gp, TN)


def chunked(kernel, steps, backward, ins, outs, scratch, name):
    def at(i):
        return steps - 1 - i if backward else i

    def spec(shape, rows):
        tail = (0,) * (len(shape) - 1)
        if rows == 0:
            return pl.BlockSpec(shape, lambda i: (0,) + tail)
        if rows < 0:
            return pl.BlockSpec((1,) + shape[1:], lambda i: (jnp.maximum(at(i) * -rows - 1, 0),) + tail)
        return pl.BlockSpec((rows,) + shape[1:], lambda i: (at(i),) + tail)

    return pl.pallas_call(
        kernel,
        grid=(steps,),
        in_specs=[spec(a.shape, r) for a, r in ins],
        out_specs=[spec(s.shape, r) for s, r in outs],
        out_shape=[s for s, _ in outs],
        scratch_shapes=scratch,
        name=name,
        compiler_params=pltpu.CompilerParams(
            dimension_semantics=("arbitrary",), vmem_limit_bytes=60 * 1024 * 1024
        ),
    )(*[a for a, _ in ins])


def on_device(
    tokens, route, cotangent, gain_mix, w_in, conv_w, w_x, w_dt, dt_bias, a_log, d_skip, w_out,
    gain_moe, w_up, w_down,
):
    n_seq, n_dp = lax.axis_size("seq"), lax.axis_size("dp")
    both = ("dp", "seq")
    here, d_model = tokens.shape
    cpd = conv_w.shape[0]
    chans = cpd * n_dp
    cp = up128(chans)
    rank = w_dt.shape[1]
    n_small = w_x.shape[1]
    sp = up128(n_small)
    tall = here * n_seq
    rows_in = w_in.shape[0]
    experts, slots = n_dp, 40

    gains = lax.all_gather(jnp.stack([gain_mix, gain_moe]), both, axis=1, tiled=True).astype(f32)
    gmix_all, gmoe_all = gains[0], gains[1]
    w_cols = w_in.reshape(rows_in, 2, n_dp, n_seq, cpd).transpose(3, 0, 1, 2, 4)
    w_cols = jnp.pad(
        w_cols.reshape(n_seq, rows_in, 2, chans), ((0, 0), (0, 0), (0, 0), (0, cp - chans))
    )
    w_cols = lax.all_to_all(w_cols.reshape(n_seq, rows_in, 2 * cp), "seq", 0, 0, tiled=True)
    w_mine = lax.all_gather(w_cols.reshape(n_seq * rows_in, 2 * cp), "dp", axis=0, tiled=True)
    packed = jnp.concatenate(
        [w_out, w_x, w_dt, conv_w, a_log, dt_bias[:, None], d_skip[:, None]], axis=1
    )
    packed = lax.all_gather(packed, "dp", axis=0, tiled=True)
    packed = jnp.pad(packed, ((0, cp - chans), (0, 0)))
    cuts = [d_model, n_small, rank, 4, NS, 1, 1]
    places = [sum(cuts[:i]) for i in range(len(cuts) + 1)]
    wout_m, wx_m, wdt_m, conv_m, alog_m, bias_m, skip_m = [
        packed[:, a:b] for a, b in zip(places[:-1], places[1:])
    ]
    wx_m = jnp.pad(wx_m, ((0, 0), (0, sp - n_small)))
    wdt_m = jnp.pad(wdt_m, ((0, 0), (0, sp - rank)))
    cw = jnp.pad(conv_m.T.astype(f32), ((0, 4), (0, 0)))
    a_neg = -jnp.exp(alog_m.astype(f32)).T
    a2 = a_neg * LOG2E
    vecs = jnp.pad(jnp.concatenate([bias_m, skip_m], axis=1).T.astype(f32), ((0, 6), (0, 0)))

    row_values = tokens.astype(f32)
    normed, norm_pullback = jax.vjp(rms_norm, row_values, gmix_all)
    normed_low = normed.astype(bf16)
    xg = lax.all_gather(normed_low, "seq", axis=0, tiled=True)
    tb = 128
    steps = tall // tb
    sds = jax.ShapeDtypeStruct
    wide = sds((tall, cp), f32)
    x, z, conv, small = chunked(
        in_kernel, steps, False,
        [(xg, tb), (w_mine, 0), (cw, 0), (wx_m, 0)],
        [(wide, tb), (wide, tb), (wide, tb), (sds((tall, sp), f32), tb)],
        [pltpu.VMEM((tb + 8, cp), f32)], "mix_in",
    )
    small = lax.psum(small, "seq")
    bct = small[:, rank:n_small].reshape(tall // 8, 8, 2 * NS).transpose(0, 2, 1)
    dtp, hs, ssm, gated, part = chunked(
        scan_kernel, steps, False,
        [(small, tb), (bct, tb // 8), (wdt_m.T, 0), (vecs, 0), (a2, 0), (conv, tb), (z, tb),
         (wout_m, 0)],
        [(wide, tb), (sds((tall, NS, cp), f32), tb), (wide, tb), (sds((tall, cp), bf16), tb),
         (sds((tall, d_model), bf16), tb)],
        [pltpu.VMEM((tb, cp), f32), pltpu.VMEM((tb, cp), f32), pltpu.VMEM((NS, cp), f32)],
        "scan_forward",
    )
    mixer_out = lax.psum_scatter(part, "seq", scatter_dimension=0, tiled=True).astype(f32)
    resid = row_values + mixer_out

    normed2, norm2_pullback = jax.vjp(rms_norm, resid, gmoe_all)
    moe_in = normed2.astype(bf16)
    choose = route[:, 0]
    onehot = (choose[:, None] == jnp.arange(experts, dtype=jnp.int32)[None, :]).astype(jnp.int32)
    slot_index = jnp.sum((jnp.cumsum(onehot, axis=0) - 1) * onehot, axis=1)
    target = choose * slots + slot_index
    pick = (target[None, :] == jnp.arange(experts * slots, dtype=jnp.int32)[:, None]).astype(bf16)

    def dispatch(values):
        send = mm(pick, values).astype(bf16).reshape(n_dp, slots, d_model)
        got = lax.all_to_all(send, "dp", 0, 0, tiled=True)
        return lax.all_gather(got.reshape(n_dp * slots, d_model), "seq", axis=0, tiled=True)

    def collect(values):
        got = lax.psum_scatter(values.astype(bf16), "seq", scatter_dimension=0, tiled=True)
        back = lax.all_to_all(got.reshape(n_dp, slots, d_model), "dp", 0, 0, tiled=True)
        return mm(pick, back.reshape(n_dp * slots, d_model), TN)

    up, down = w_up[0], w_down[0]
    grad_slots = dispatch(cotangent)
    grad_hidden = mm(grad_slots, down, NT)
    slot_rows = dispatch(moe_in)
    pre_act = mm(slot_rows, up, NT)
    hidden_f, gelu_pullback = jax.vjp(partial(jax.nn.gelu, approximate=False), pre_act)
    hidden = hidden_f.astype(bf16)
    grad_pre = gelu_pullback(grad_hidden)[0].astype(bf16)
    grad_moe_in = collect(mm(grad_pre, up))
    result = (resid + collect(mm(hidden, down))).astype(bf16)
    grad_down = mm(hidden, grad_slots, TN)
    grad_up = mm(grad_pre, slot_rows, TN)

    grad_resid, grad_gmoe = norm2_pullback(grad_moe_in)
    grad_resid = grad_resid + cotangent.astype(f32)
    gml = lax.all_gather(grad_resid.astype(bf16), "seq", axis=0, tiled=True)
    grad_rank, gbct, gu, gz, gwout, gwdt, ga, gvecs = chunked(
        back_kernel, steps, True,
        [(gml, tb), (wout_m, 0), (gated, tb), (conv, tb), (z, tb), (ssm, tb), (dtp, tb), (hs, tb),
         (hs, -tb), (bct, tb // 8), (small, tb), (wdt_m, 0), (vecs, 0), (a2, 0)],
        [(sds((tall, sp), f32), tb), (sds((tall // 8, 2 * NS, 8), f32), tb // 8), (wide, tb),
         (sds((tall, cp), bf16), tb), (sds((cp, d_model), f32), 0), (sds((cp, sp), f32), 0),
         (sds((NS, cp), f32), 0), (sds((8, cp), f32), 0)],
        [pltpu.VMEM((tb, cp), f32) for _ in range(5)] + [pltpu.VMEM((NS, cp), f32)],
        "scan_backward",
    )
    grad_bc = gbct.transpose(0, 2, 1).reshape(tall, 2 * NS)
    gsmall = jnp.concatenate([grad_rank[:, :rank], grad_bc], axis=1)
    gsmall = lax.psum(jnp.pad(gsmall, ((0, 0), (0, sp - n_small))), "seq")
    gpart, gwx, gw, gcw = chunked(
        out_kernel, steps, True,
        [(gsmall, tb), (wx_m, 0), (conv, tb), (x, tb), (gu, tb), (gz, tb), (xg, tb), (w_mine, 0),
         (cw, 0)],
        [(sds((tall, d_model), bf16), tb), (sds((cp, sp), f32), 0),
         (sds((d_model, 2 * cp), f32), 0), (sds((8, cp), f32), 0)],
        [pltpu.VMEM((tb + 8, cp), f32)], "mix_out",
    )
    grad_normed = lax.psum_scatter(gpart, "seq", scatter_dimension=0, tiled=True).astype(f32)
    grad_row_norm, grad_gmix = norm_pullback(grad_normed)
    grad_tokens = grad_row_norm + grad_resid

    ggains = lax.psum_scatter(
        jnp.stack([grad_gmix, grad_gmoe]), both, scatter_dimension=1, tiled=True
    )
    gw = gw.reshape(d_model, 2, cp)[:, :, :chans].reshape(d_model, 2 * chans).astype(bf16)
    gw = lax.psum_scatter(gw, "dp", scatter_dimension=0, tiled=True)
    gw = lax.all_to_all(gw.reshape(n_seq, rows_in, 2 * chans), "seq", 0, 0, tiled=True)
    gw = gw.reshape(n_seq, rows_in, 2, n_dp, cpd).transpose(1, 2, 3, 0, 4)
    grad_win = gw.reshape(rows_in, 2 * n_dp * n_seq * cpd).astype(f32)
    gpack = jnp.concatenate(
        [gwx[:, :n_small], gwdt[:, :rank], gcw[:4].T, (ga * a_neg).T, gvecs[:2].T], axis=1
    )[:chans]
    gpack = lax.psum_scatter(gpack, "dp", scatter_dimension=0, tiled=True)
    grad_wout = lax.psum_scatter(
        gwout[:chans].astype(bf16), "dp", scatter_dimension=0, tiled=True
    ).astype(f32)
    edges = [p - d_model for p in places[1:]]
    gwx_m, gwdt_m, gconv_m, galog_m, gbias_m, gskip_m = [
        gpack[:, a:b] for a, b in zip(edges[:-1], edges[1:])
    ]
    return (
        result, grad_tokens, ggains[0], grad_win, gconv_m, gwx_m, gwdt_m, gbias_m[:, 0], galog_m,
        gskip_m[:, 0], grad_wout, ggains[1], grad_up[None], grad_down[None],
    )


def solution(mesh):
    row2, row1 = P(("dp", "seq"), None), P(("dp", "seq"))
    mats = P("dp", "seq", None)
    return jax.shard_map(
        on_device,
        mesh=mesh,
        in_specs=(
            row2, row2, row2, row1, row2, row2, row2, row2, row1, row2, row1, row2, row1, mats, mats
        ),
        out_specs=(
            row2, row2, row1, row2, row2, row2, row2, row1, row2, row1, row2, row1, mats, mats
        ),
        check_vma=False,
    )
```

```python
from functools import partial

import jax
import jax.numpy as jnp
from jax import lax
from jax.experimental import pallas as pl
from jax.experimental.pallas import tpu as pltpu
from jax.sharding import PartitionSpec as P

NS = 16
LN2 = 0.6931471805599453
LOG2E = 1.4426950408889634
eps = 1e-05
f32 = jnp.float32
bf16 = jnp.bfloat16

NN = (((1,), (0,)), ((), ()))
NT = (((1,), (1,)), ((), ()))
TN = (((0,), (0,)), ((), ()))


def mm(left, right, dims=NN):
    return lax.dot_general(left, right, dims, preferred_element_type=f32)


def up128(count):
    return -(-count // 128) * 128


def rms_norm(values, gain_vec):
    return values * lax.rsqrt(jnp.mean(values * values, axis=-1, keepdims=True) + eps) * gain_vec


def sigmoid(v):
    return 1.0 / (1.0 + jnp.exp(-v))


def softplus(v):
    return jnp.maximum(v, 0.0) + jnp.log1p(jnp.exp(-jnp.abs(v)))


def tree_step(first, second, by):
    row = lax.broadcasted_iota(jnp.int32, first.shape, 0)
    clear = (row & by) == 0
    return jnp.where(clear, first, second) + pltpu.roll(jnp.where(clear, second, first), by, 0)


def tree_push(stack, value, falling=False):
    level = 1
    while stack and stack[-1][0] == level:
        other = stack.pop()[1]
        value = tree_step(value, other, level) if falling else tree_step(other, value, level)
        level *= 2
    stack.append((level, value))


def in_kernel(xg, w, cw, wx, x_out, z_out, conv_out, small_out, buf):
    rows, cp = x_out.shape

    @pl.when(pl.program_id(0) == 0)
    def _():
        buf[0:8, :] = jnp.zeros((8, cp), f32)

    @pl.when(pl.program_id(0) > 0)
    def _():
        buf[0:8, :] = buf[rows : rows + 8, :]

    prod = mm(xg[...], w[...])
    x_part = prod[:, :cp]
    x_out[...] = x_part
    z_out[...] = prod[:, cp:]
    buf[8 : 8 + rows, :] = x_part
    conv = x_part * cw[3:4, :]
    for k in range(3):
        conv = conv + buf[5 + k : 5 + k + rows, :] * cw[k : k + 1, :]
    conv_out[...] = conv
    small_out[...] = mm((conv * sigmoid(conv)).astype(bf16), wx[...])


def scan_kernel(
    small, bct, wdtt, vecs, a2, conv, z, wout, dtp_out, h_out, ssm_out, gated_out, part_out,
    delta_s, du_s, state,
):
    rows, cp = conv.shape

    @pl.when(pl.program_id(0) == 0)
    def _():
        state[...] = jnp.zeros_like(state)

    dtp = mm(small[...].astype(bf16), wdtt[...]) + vecs[0:1, :]
    dtp_out[...] = dtp
    delta = softplus(dtp)
    cv = conv[...]
    u = cv * sigmoid(cv)
    delta_s[...] = delta
    du_s[...] = delta * u

    def group(g, h):
        base = pl.multiple_of(g * 8, 8)
        bc = bct[g]
        stack = []
        for t in range(8):
            d = jnp.broadcast_to(delta_s[pl.ds(base + t, 1), :], (NS, cp))
            du = jnp.broadcast_to(du_s[pl.ds(base + t, 1), :], (NS, cp))
            h = jnp.exp2(d * a2[...]) * h + du * bc[:NS, t : t + 1]
            h_out[base + t] = h
            prod = h * bc[NS:, t : t + 1]
            tree_push(stack, prod[:8] + prod[8:])
        ssm_out[pl.ds(base, 8), :] = stack[0][1]
        return h

    state[...] = lax.fori_loop(0, rows // 8, group, state[...])
    zv = z[...]
    gated = (ssm_out[...] + vecs[1:2, :] * u) * (zv * sigmoid(zv))
    low = gated.astype(bf16)
    gated_out[...] = low
    part_out[...] = mm(low, wout[...]).astype(part_out.dtype)


def back_kernel(
    gml, wout, gated, conv, z, ssm, dtp, hs, hlast, bct, small, wdt, vecs, a2,
    rank_out, gbct_out, gu_out, gz_out, gwout, gwdt, ga, gvecs,
    delta_s, du_s, gs_s, r1_s, r2_s, lam_s,
):
    rows, cp = conv.shape
    step = pl.program_id(0)
    last = pl.num_programs(0) - 1

    @pl.when(step == 0)
    def _():
        lam_s[...] = jnp.zeros_like(lam_s)
        gwout[...] = jnp.zeros_like(gwout)
        gwdt[...] = jnp.zeros_like(gwdt)
        ga[...] = jnp.zeros_like(ga)
        gvecs[...] = jnp.zeros_like(gvecs)

    grad_mixed = gml[...]
    gg = mm(grad_mixed, wout[...], NT)
    gwout[...] += mm(gated[...], grad_mixed, TN)
    zv = z[...]
    sz = sigmoid(zv)
    cv = conv[...]
    u = cv * sigmoid(cv)
    skip = vecs[1:2, :]
    gz_out[...] = (gg * (ssm[...] + skip * u) * (sz * (1.0 + zv * (1.0 - sz)))).astype(bf16)
    gs = gg * (zv * sz)
    delta = softplus(dtp[...])
    gs_s[...] = gs
    delta_s[...] = delta
    du_s[...] = delta * u
    lane = lax.broadcasted_iota(jnp.int32, (NS, 128), 1)
    keep_first = jnp.where(step == last, 0.0, 1.0)
    tiles = cp // 128

    def lane_fold(v):
        total = v[:, :128]
        for i in range(1, tiles):
            total = total + v[:, i * 128 : (i + 1) * 128]
        return jnp.sum(total, axis=1, keepdims=True)

    def group(k, carry):
        lamd, acc = carry
        g = rows // 8 - 1 - k
        base = pl.multiple_of(g * 8, 8)
        bc = bct[g]
        stack1, stack2 = [], []
        gb = jnp.zeros((NS, 128), f32)
        gc = jnp.zeros((NS, 128), f32)
        h = hs[base + 7]
        ones, twos = {}, {}
        for t in range(7, -1, -1):
            d = jnp.broadcast_to(delta_s[pl.ds(base + t, 1), :], (NS, cp))
            du = jnp.broadcast_to(du_s[pl.ds(base + t, 1), :], (NS, cp))
            g_s = jnp.broadcast_to(gs_s[pl.ds(base + t, 1), :], (NS, cp))
            if t > 0:
                before = hs[base + t - 1]
            else:
                inside = hs[jnp.maximum(base - 1, 0)]
                before = jnp.where(g == 0, hlast[0] * keep_first, inside)
            lam = lamd + g_s * bc[NS:, t : t + 1]
            gc = jnp.where(lane == t, lane_fold(g_s * h), gc)
            gb = jnp.where(lane == t, lane_fold(lam * du), gb)
            lamd = jnp.exp2(d * a2[...]) * lam
            w = lamd * before
            acc = acc + w * d
            wa = w * a2[...]
            lb = lam * bc[:NS, t : t + 1]
            tree_push(stack1, wa[:8] + wa[8:], True)
            tree_push(stack2, lb[:8] + lb[8:], True)
            h = before
        r1_s[pl.ds(base, 8), :] = stack1[0][1]
        r2_s[pl.ds(base, 8), :] = stack2[0][1]
        gbct_out[g, :NS, :] = gb[:, :8]
        gbct_out[g, NS:, :] = gc[:, :8]
        return lamd, acc

    lamd, acc = lax.fori_loop(0, rows // 8, group, (lam_s[...], jnp.zeros((NS, cp), f32)))
    lam_s[...] = lamd
    ga[...] += acc
    r2 = r2_s[...]
    gu_out[...] = skip * gs + delta * r2
    gdelta = r1_s[...] * LN2 + u * r2
    gdtp = gdelta * sigmoid(dtp[...])
    gvecs[0:1, :] += jnp.sum(gdtp, axis=0, keepdims=True)
    gvecs[1:2, :] += jnp.sum(gs * u, axis=0, keepdims=True)
    low = gdtp.astype(bf16)
    gwdt[...] += mm(low, small[...].astype(bf16), TN)
    rank_out[...] = mm(low, wdt[...])


def out_kernel(
    gsmall, wx, conv, x, gu, gz, xg, w, cw, part_out, gwx, gw, gcw, buf
):
    rows, cp = conv.shape

    @pl.when(pl.program_id(0) == 0)
    def _():
        buf[rows : rows + 8, :] = jnp.zeros((8, cp), f32)
        gwx[...] = jnp.zeros_like(gwx)
        gw[...] = jnp.zeros_like(gw)
        gcw[...] = jnp.zeros_like(gcw)

    @pl.when(pl.program_id(0) > 0)
    def _():
        buf[rows : rows + 8, :] = buf[0:8, :]

    gsl = gsmall[...].astype(bf16)
    cv = conv[...]
    s = sigmoid(cv)
    gwx[...] += mm((cv * s).astype(bf16), gsl, TN)
    gconv = (gu[...] + mm(gsl, wx[...], NT)) * (s * (1.0 + cv * (1.0 - s)))
    buf[0:rows, :] = gconv
    xv = x[...]
    gx = gconv * cw[3:4, :]
    gcw[3:4, :] += jnp.sum(gconv * xv, axis=0, keepdims=True)
    for k in range(3):
        moved = buf[3 - k : 3 - k + rows, :]
        gx = gx + moved * cw[k : k + 1, :]
        gcw[k : k + 1, :] += jnp.sum(moved * xv, axis=0, keepdims=True)
    gp = jnp.concatenate([gx.astype(bf16), gz[...]], axis=1)
    part_out[...] = mm(gp, w[...], NT).astype(part_out.dtype)
    gw[...] += mm(xg[...], gp, TN)


def chunked(kernel, steps, backward, ins, outs, scratch, name):
    def at(i):
        return steps - 1 - i if backward else i

    def spec(shape, rows):
        tail = (0,) * (len(shape) - 1)
        if rows == 0:
            return pl.BlockSpec(shape, lambda i: (0,) + tail)
        if rows < 0:
            return pl.BlockSpec((1,) + shape[1:], lambda i: (jnp.maximum(at(i) * -rows - 1, 0),) + tail)
        return pl.BlockSpec((rows,) + shape[1:], lambda i: (at(i),) + tail)

    return pl.pallas_call(
        kernel,
        grid=(steps,),
        in_specs=[spec(a.shape, r) for a, r in ins],
        out_specs=[spec(s.shape, r) for s, r in outs],
        out_shape=[s for s, _ in outs],
        scratch_shapes=scratch,
        name=name,
        compiler_params=pltpu.CompilerParams(
            dimension_semantics=("arbitrary",), vmem_limit_bytes=60 * 1024 * 1024
        ),
    )(*[a for a, _ in ins])


MESH = pl.DeviceIdType.MESH


def remote(src, dst, send, recv, **where):
    return pltpu.make_async_remote_copy(
        src_ref=src, dst_ref=dst, send_sem=send, recv_sem=recv, device_id=where, device_id_type=MESH
    )


class Line:
    def __init__(self, n_seq):
        assert n_seq % 2 == 0
        self.n = n_seq // 2
        self.n_seq = n_seq
        self.me = lax.axis_index("seq")
        self.o, self.i = self.me // 2, self.me % 2

    def at(self, o, i):
        return o * 2 + i

    def neighbours(self):
        return [
            (None, self.at(self.o, 1 - self.i)),
            (self.o > 0, self.at(self.o - 1, self.i)),
            (self.o < self.n - 1, self.at(self.o + 1, self.i)),
        ]

    def order(self, t):
        table = [
            sorted(range(self.n), key=lambda q, o=o: (-abs(q - o), -q))[t] for o in range(self.n)
        ]
        place = jnp.int32(0)
        for o in range(self.n):
            place = place + jnp.where(self.o == o, table[o], 0)
        return place


def when(condition, action):
    if condition is None:
        action()
    else:
        pl.when(condition)(action)


def greet(peers, extra=()):
    barrier = pltpu.get_barrier_semaphore()
    count = jnp.int32(0)
    for condition, place in peers:
        when(
            condition,
            lambda place=place: pl.semaphore_signal(
                barrier, inc=1, device_id={"seq": place}, device_id_type=MESH
            ),
        )
        count = count + (1 if condition is None else jnp.where(condition, 1, 0))
    for place in extra:
        pl.semaphore_signal(barrier, inc=1, device_id={"dp": place}, device_id_type=MESH)
        count = count + 1
    pl.semaphore_wait(barrier, count)


def gather_sems(n, pieces):
    dma = pltpu.SemaphoreType.DMA
    return [dma((n, pieces)), dma((pieces,)), dma((n, pieces)), dma((n, pieces)), dma((n, pieces))]


def gather(line, out, own, pieces, sems, ready=None):
    zs, zd, zr, ys, yr = sems
    sent = []
    o, i, n = line.o, line.i, line.n

    def go(condition, copy):
        when(condition, lambda: copy.start())
        sent.append((condition, copy))

    def both(a, b):
        return b if a is None else jnp.logical_and(a, b)

    def spread(condition, src, p, q, up, down, down_sem):
        slot = line.at(q, i)
        if up:
            go(both(condition, o < n - 1),
               remote(src, out.at[slot, p], zs.at[q, p], zr.at[q, p], seq=line.at(o + 1, i)))
        if down:
            go(both(condition, o > 0),
               remote(src, out.at[slot, p], down_sem, zr.at[q, p], seq=line.at(o - 1, i)))
        go(condition, remote(src, out.at[slot, p], ys.at[q, p], yr.at[q, p], seq=line.at(o, 1 - i)))

    for p in pieces:
        if ready is not None:
            ready(p)
        spread(None, own(p), p, o, True, True, zd.at[p])
    for k in range(1, n):
        for p in pieces:
            for q, condition, up in ((o - k, o >= k, True), (o + k, o + k <= n - 1, False)):
                here = out.at[line.at(q, i), p]

                def arrive(here=here, q=q, p=p):
                    remote(here, here, zs.at[q, p], zr.at[q, p], seq=line.at(o, 1 - i)).wait_recv()

                when(condition, arrive)
                spread(condition, here, p, q, up, not up, zs.at[q, p])
    for q in range(n):
        for p in pieces:
            here = out.at[line.at(q, 1 - i), p]
            remote(here, here, ys.at[q, p], yr.at[q, p], seq=line.at(o, 1 - i)).wait_recv()
    for condition, copy in sent:
        when(condition, lambda copy=copy: copy.wait_send())


def gather_kernel(n_seq, x, out, lsem, *sems):
    line = Line(n_seq)
    greet(line.neighbours())
    keep = pltpu.make_async_copy(x, out.at[line.me], lsem)
    keep.start()
    gather(line, out, lambda p: x.at[p], range(x.shape[0]), sems)
    keep.wait()


def seq_gather(x, n_seq, pieces, number):
    rows, width = x.shape
    out = pl.pallas_call(
        partial(gather_kernel, n_seq),
        in_specs=[pl.BlockSpec(memory_space=pl.ANY)],
        out_specs=pl.BlockSpec(memory_space=pl.ANY),
        out_shape=jax.ShapeDtypeStruct((n_seq, pieces, rows // pieces, width), x.dtype),
        scratch_shapes=[pltpu.SemaphoreType.DMA] + gather_sems(n_seq // 2, pieces),
        compiler_params=pltpu.CompilerParams(collective_id=number, has_side_effects=True),
        name="seq_gather",
    )(x.reshape(pieces, rows // pieces, width))
    return out.reshape(n_seq * rows, width)


def dispatch_kernel(n_seq, n_dp, x, out, lsem, dps, dpr, *sems):
    line = Line(n_seq)
    mine = lax.axis_index("dp")
    peers = [lax.rem(mine + r, n_dp) for r in range(1, n_dp)]
    greet(line.neighbours(), peers)
    copies = []
    for r, peer in enumerate(peers):
        copy = remote(x.at[peer], out.at[line.me, mine], dps.at[r], dpr.at[r], dp=peer)
        copy.start()
        copies.append(copy)
    keep = pltpu.make_async_copy(x.at[mine], out.at[line.me, mine], lsem)
    keep.start()

    def ready(r):
        if r == 0:
            keep.wait()
        else:
            source = out.at[line.me, lax.rem(mine + n_dp - r, n_dp)]
            remote(source, source, dps.at[r - 1], dpr.at[r - 1], dp=peers[r - 1]).wait_recv()

    gather_rolled(line, out, mine, n_dp, sems, ready)
    for copy in copies:
        copy.wait_send()


class Rolled:
    def __init__(self, out, mine, n_dp):
        self.out, self.mine, self.n_dp = out, mine, n_dp

    @property
    def at(self):
        return self

    def __getitem__(self, key):
        slot, r = key
        return self.out.at[slot, lax.rem(self.mine + self.n_dp - r, self.n_dp)]


def gather_rolled(line, out, mine, n_dp, sems, ready):
    view = Rolled(out, mine, n_dp)
    gather(line, view, lambda r: view.at[line.me, r], range(n_dp), sems, ready)


def dispatch_call(x, n_seq, number):
    n_dp, rows, width = x.shape
    dma = pltpu.SemaphoreType.DMA
    return pl.pallas_call(
        partial(dispatch_kernel, n_seq, n_dp),
        in_specs=[pl.BlockSpec(memory_space=pl.ANY)],
        out_specs=pl.BlockSpec(memory_space=pl.ANY),
        out_shape=jax.ShapeDtypeStruct((n_seq, n_dp, rows, width), x.dtype),
        scratch_shapes=[dma, dma((n_dp - 1,)), dma((n_dp - 1,))] + gather_sems(n_seq // 2, n_dp),
        compiler_params=pltpu.CompilerParams(collective_id=number, has_side_effects=True),
        name="dispatch",
    )(x)


def scatter_scratch(n, pieces, rows, width):
    dma = pltpu.SemaphoreType.DMA
    return [
        pltpu.VMEM((n, pieces, rows, width), bf16),
        pltpu.VMEM((n, pieces, rows, width), bf16),
        pltpu.VMEM((n + 1, pieces, rows, width), bf16),
        dma((n, pieces)), dma((n, pieces)), dma((n, pieces)), dma((n + 1, pieces)),
    ]


def scatter(line, term, pieces, scratch, final):
    ybuf, zout, zin, ys, yr, zs, zr = scratch
    o, i, n = line.o, line.i, line.n
    sent = []
    orders = [line.order(t) for t in range(n)]
    for q in orders:
        for p in pieces:
            copy = remote(term.at[line.at(q, 1 - i), p], ybuf.at[q, p], ys.at[q, p], yr.at[q, p],
                          seq=line.at(o, 1 - i))
            copy.start()
            sent.append(copy)

    def arrived(k, p):
        remote(zin.at[k, p], zin.at[k, p], zs.at[0, p], zr.at[k, p], seq=line.at(o, 1 - i)).wait_recv()

    for t, q in enumerate(orders):
        for p in pieces:
            remote(ybuf.at[q, p], ybuf.at[q, p], ys.at[q, p], yr.at[q, p],
                   seq=line.at(o, 1 - i)).wait_recv()
            value = term[line.at(q, i), p].astype(f32) + ybuf[q, p].astype(f32)
            if t < n - 1:
                up = q > o
                fed = jnp.where(up, o > 0, o < n - 1)

                def with_feed(q=q, p=p, value=value):
                    arrived(q, p)
                    zout[q, p] = (value + zin[q, p].astype(f32)).astype(bf16)

                def without(q=q, p=p, value=value):
                    zout[q, p] = value.astype(bf16)

                pl.when(fed)(with_feed)
                pl.when(jnp.logical_not(fed))(without)
                to = jnp.where(up, o + 1, o - 1)
                slot = jnp.where(jnp.logical_and(q == to, jnp.logical_not(up)), n, q)
                copy = remote(zout.at[q, p], zin.at[slot, p], zs.at[q, p], zr.at[slot, p],
                              seq=line.at(to, i))
                copy.start()
                sent.append(copy)
            else:
                below, above = o > 0, o < n - 1
                pl.when(below)(lambda p=p: arrived(o, p))
                pl.when(above)(lambda p=p: arrived(n, p))
                value = value + jnp.where(below, zin[o, p].astype(f32), 0.0)
                value = value + jnp.where(above, zin[n, p].astype(f32), 0.0)
                final(p, value)
    for copy in sent:
        copy.wait_send()


def scatter_kernel(n_seq, term, out, *scratch):
    line = Line(n_seq)
    greet(line.neighbours())

    def final(p, value):
        out[p] = value

    scatter(line, term, range(term.shape[1]), scratch, final)


def seq_scatter(x, n_seq, pieces, number):
    rows, width = x.shape[0] // n_seq, x.shape[1]
    part = rows // pieces
    vmem = pl.BlockSpec(memory_space=pltpu.VMEM)
    out = pl.pallas_call(
        partial(scatter_kernel, n_seq),
        in_specs=[vmem],
        out_specs=vmem,
        out_shape=jax.ShapeDtypeStruct((pieces, part, width), f32),
        scratch_shapes=scatter_scratch(n_seq // 2, pieces, part, width),
        compiler_params=pltpu.CompilerParams(
            collective_id=number, has_side_effects=True, vmem_limit_bytes=60 * 1024 * 1024
        ),
        name="seq_scatter",
    )(x.reshape(n_seq, pieces, part, width))
    return out.reshape(rows, width)


def collect_kernel(n_seq, n_dp, term, out, sumbuf, lsem, dps, dpr, *scratch):
    line = Line(n_seq)
    mine = lax.axis_index("dp")
    peers = [lax.rem(mine + r, n_dp) for r in range(1, n_dp)]
    greet(line.neighbours(), peers)
    copies = []
    view = RolledTerm(term, mine, n_dp)

    def final(r, value):
        sumbuf[r] = value.astype(bf16)
        if r == 0:
            copy = pltpu.make_async_copy(sumbuf.at[0], out.at[mine], lsem)
        else:
            copy = remote(sumbuf.at[r], out.at[mine], dps.at[r - 1], dpr.at[r - 1], dp=peers[r - 1])
        copy.start()
        copies.append(copy)

    scatter(line, view, list(range(1, n_dp)) + [0], scratch, final)
    for r in range(1, n_dp):
        here = out.at[lax.rem(mine + n_dp - r, n_dp)]
        remote(here, here, dps.at[r - 1], dpr.at[r - 1], dp=peers[r - 1]).wait_recv()
    copies[-1].wait()
    for copy in copies[:-1]:
        copy.wait_send()


class RolledTerm:
    def __init__(self, term, mine, n_dp):
        self.term, self.mine, self.n_dp = term, mine, n_dp

    def index(self, key):
        return key[0], lax.rem(self.mine + key[1], self.n_dp)

    def __getitem__(self, key):
        return self.term[self.index(key)]

    @property
    def at(self):
        class View:
            def __getitem__(view, key):
                return self.term.at[self.index(key)]

        return View()


def collect_call(x, n_seq, number):
    _, n_dp, rows, width = x.shape
    dma = pltpu.SemaphoreType.DMA
    vmem = pl.BlockSpec(memory_space=pltpu.VMEM)
    return pl.pallas_call(
        partial(collect_kernel, n_seq, n_dp),
        in_specs=[vmem],
        out_specs=vmem,
        out_shape=jax.ShapeDtypeStruct((n_dp, rows, width), bf16),
        scratch_shapes=[pltpu.VMEM((n_dp, rows, width), bf16), dma, dma((n_dp - 1,)), dma((n_dp - 1,))]
        + scatter_scratch(n_seq // 2, n_dp, rows, width),
        compiler_params=pltpu.CompilerParams(
            collective_id=number, has_side_effects=True, vmem_limit_bytes=60 * 1024 * 1024
        ),
        name="collect",
    )(x)


def sum_kernel(n_seq, x, out, inbox, total, lsem, s1, r1, s2, r2):
    me = lax.axis_index("seq")
    peers = [lax.rem(me + r, n_seq) for r in range(1, n_seq)]
    greet([(None, q) for q in peers])
    copies = []
    for r, q in enumerate(peers):
        copy = remote(x.at[q], inbox.at[r], s1.at[r], r1.at[r], seq=q)
        copy.start()
        copies.append(copy)
    value = x[me].astype(f32)
    for r, q in enumerate(peers):
        remote(inbox.at[r], inbox.at[r], s1.at[r], r1.at[r], seq=q).wait_recv()
        value = value + inbox[r].astype(f32)
    total[...] = value.astype(total.dtype)
    for r, q in enumerate(peers):
        copy = remote(total, out.at[me], s2.at[r], r2.at[r], seq=q)
        copy.start()
        copies.append(copy)
    keep = pltpu.make_async_copy(total, out.at[me], lsem)
    keep.start()
    for r, q in enumerate(peers):
        here = out.at[lax.rem(me + n_seq - 1 - r, n_seq)]
        remote(here, here, s2.at[r], r2.at[r], seq=q).wait_recv()
    keep.wait()
    for copy in copies:
        copy.wait_send()


def seq_sum(x, n_seq, number):
    rows, width = x.shape[0] // n_seq, x.shape[1]
    dma = pltpu.SemaphoreType.DMA
    vmem = pl.BlockSpec(memory_space=pltpu.VMEM)
    out = pl.pallas_call(
        partial(sum_kernel, n_seq),
        in_specs=[vmem],
        out_specs=vmem,
        out_shape=jax.ShapeDtypeStruct((n_seq, rows, width), x.dtype),
        scratch_shapes=[pltpu.VMEM((n_seq - 1, rows, width), x.dtype), pltpu.VMEM((rows, width), x.dtype),
                        dma] + [dma((n_seq - 1,)) for _ in range(4)],
        compiler_params=pltpu.CompilerParams(
            collective_id=number, has_side_effects=True, vmem_limit_bytes=60 * 1024 * 1024
        ),
        name="seq_sum",
    )(x.reshape(n_seq, rows, width))
    return out.reshape(n_seq * rows, width)


def on_device(
    tokens, route, cotangent, gain_mix, w_in, conv_w, w_x, w_dt, dt_bias, a_log, d_skip, w_out,
    gain_moe, w_up, w_down,
):
    n_seq, n_dp = lax.axis_size("seq"), lax.axis_size("dp")
    both = ("dp", "seq")
    here, d_model = tokens.shape
    cpd = conv_w.shape[0]
    chans = cpd * n_dp
    cp = up128(chans)
    rank = w_dt.shape[1]
    n_small = w_x.shape[1]
    sp = up128(n_small)
    tall = here * n_seq
    rows_in = w_in.shape[0]
    experts, slots = n_dp, 40

    gains = lax.all_gather(jnp.stack([gain_mix, gain_moe]), both, axis=1, tiled=True).astype(f32)
    gmix_all, gmoe_all = gains[0], gains[1]
    w_cols = w_in.reshape(rows_in, 2, n_dp, n_seq, cpd).transpose(3, 0, 1, 2, 4)
    w_cols = jnp.pad(
        w_cols.reshape(n_seq, rows_in, 2, chans), ((0, 0), (0, 0), (0, 0), (0, cp - chans))
    )
    w_cols = lax.all_to_all(w_cols.reshape(n_seq, rows_in, 2 * cp), "seq", 0, 0, tiled=True)
    w_mine = lax.all_gather(w_cols.reshape(n_seq * rows_in, 2 * cp), "dp", axis=0, tiled=True)
    packed = jnp.concatenate(
        [w_out, w_x, w_dt, conv_w, a_log, dt_bias[:, None], d_skip[:, None]], axis=1
    )
    packed = lax.all_gather(packed, "dp", axis=0, tiled=True)
    packed = jnp.pad(packed, ((0, cp - chans), (0, 0)))
    cuts = [d_model, n_small, rank, 4, NS, 1, 1]
    places = [sum(cuts[:i]) for i in range(len(cuts) + 1)]
    wout_m, wx_m, wdt_m, conv_m, alog_m, bias_m, skip_m = [
        packed[:, a:b] for a, b in zip(places[:-1], places[1:])
    ]
    wx_m = jnp.pad(wx_m, ((0, 0), (0, sp - n_small)))
    wdt_m = jnp.pad(wdt_m, ((0, 0), (0, sp - rank)))
    cw = jnp.pad(conv_m.T.astype(f32), ((0, 4), (0, 0)))
    a_neg = -jnp.exp(alog_m.astype(f32)).T
    a2 = a_neg * LOG2E
    vecs = jnp.pad(jnp.concatenate([bias_m, skip_m], axis=1).T.astype(f32), ((0, 6), (0, 0)))

    row_values = tokens.astype(f32)
    normed, norm_pullback = jax.vjp(rms_norm, row_values, gmix_all)
    normed_low = normed.astype(bf16)
    xg = seq_gather(normed_low, n_seq, 2, 0)
    tb = 128
    steps = tall // tb
    sds = jax.ShapeDtypeStruct
    wide = sds((tall, cp), f32)
    x, z, conv, small = chunked(
        in_kernel, steps, False,
        [(xg, tb), (w_mine, 0), (cw, 0), (wx_m, 0)],
        [(wide, tb), (wide, tb), (wide, tb), (sds((tall, sp), f32), tb)],
        [pltpu.VMEM((tb + 8, cp), f32)], "mix_in",
    )
    small = seq_sum(small.astype(bf16), n_seq, 1).astype(f32)
    bct = small[:, rank:n_small].reshape(tall // 8, 8, 2 * NS).transpose(0, 2, 1)
    dtp, hs, ssm, gated, part = chunked(
        scan_kernel, steps, False,
        [(small, tb), (bct, tb // 8), (wdt_m.T, 0), (vecs, 0), (a2, 0), (conv, tb), (z, tb),
         (wout_m, 0)],
        [(wide, tb), (sds((tall, NS, cp), f32), tb), (wide, tb), (sds((tall, cp), bf16), tb),
         (sds((tall, d_model), bf16), tb)],
        [pltpu.VMEM((tb, cp), f32), pltpu.VMEM((tb, cp), f32), pltpu.VMEM((NS, cp), f32)],
        "scan_forward",
    )
    mixer_out = seq_scatter(part, n_seq, 2, 2)
    resid = row_values + mixer_out

    normed2, norm2_pullback = jax.vjp(rms_norm, resid, gmoe_all)
    moe_in = normed2.astype(bf16)
    choose = route[:, 0]
    onehot = (choose[:, None] == jnp.arange(experts, dtype=jnp.int32)[None, :]).astype(jnp.int32)
    slot_index = jnp.sum((jnp.cumsum(onehot, axis=0) - 1) * onehot, axis=1)
    target = choose * slots + slot_index
    pick = (target[None, :] == jnp.arange(experts * slots, dtype=jnp.int32)[:, None]).astype(bf16)

    def dispatch(values, number):
        send = mm(pick, values).astype(bf16).reshape(n_dp, slots, d_model)
        return dispatch_call(send, n_seq, number).reshape(n_seq * n_dp * slots, d_model)

    def collect(values, number):
        values = values.astype(bf16).reshape(n_seq, n_dp, slots, d_model)
        return mm(pick, collect_call(values, n_seq, number).reshape(n_dp * slots, d_model), TN)

    up, down = w_up[0], w_down[0]
    grad_slots = dispatch(cotangent, 3)
    grad_hidden = mm(grad_slots, down, NT)
    slot_rows = dispatch(moe_in, 4)
    pre_act = mm(slot_rows, up, NT)
    hidden_f, gelu_pullback = jax.vjp(partial(jax.nn.gelu, approximate=False), pre_act)
    hidden = hidden_f.astype(bf16)
    grad_pre = gelu_pullback(grad_hidden)[0].astype(bf16)
    grad_moe_in = collect(mm(grad_pre, up), 5)
    result = (resid + collect(mm(hidden, down), 6)).astype(bf16)
    grad_down = mm(hidden, grad_slots, TN)
    grad_up = mm(grad_pre, slot_rows, TN)

    grad_resid, grad_gmoe = norm2_pullback(grad_moe_in)
    grad_resid = grad_resid + cotangent.astype(f32)
    gml = seq_gather(grad_resid.astype(bf16), n_seq, 2, 7)
    grad_rank, gbct, gu, gz, gwout, gwdt, ga, gvecs = chunked(
        back_kernel, steps, True,
        [(gml, tb), (wout_m, 0), (gated, tb), (conv, tb), (z, tb), (ssm, tb), (dtp, tb), (hs, tb),
         (hs, -tb), (bct, tb // 8), (small, tb), (wdt_m, 0), (vecs, 0), (a2, 0)],
        [(sds((tall, sp), f32), tb), (sds((tall // 8, 2 * NS, 8), f32), tb // 8), (wide, tb),
         (sds((tall, cp), bf16), tb), (sds((cp, d_model), f32), 0), (sds((cp, sp), f32), 0),
         (sds((NS, cp), f32), 0), (sds((8, cp), f32), 0)],
        [pltpu.VMEM((tb, cp), f32) for _ in range(5)] + [pltpu.VMEM((NS, cp), f32)],
        "scan_backward",
    )
    grad_bc = gbct.transpose(0, 2, 1).reshape(tall, 2 * NS)
    gsmall = jnp.concatenate([grad_rank[:, :rank], grad_bc], axis=1)
    gsmall = seq_sum(jnp.pad(gsmall, ((0, 0), (0, sp - n_small))).astype(bf16), n_seq, 8)
    gpart, gwx, gw, gcw = chunked(
        out_kernel, steps, True,
        [(gsmall, tb), (wx_m, 0), (conv, tb), (x, tb), (gu, tb), (gz, tb), (xg, tb), (w_mine, 0),
         (cw, 0)],
        [(sds((tall, d_model), bf16), tb), (sds((cp, sp), f32), 0),
         (sds((d_model, 2 * cp), f32), 0), (sds((8, cp), f32), 0)],
        [pltpu.VMEM((tb + 8, cp), f32)], "mix_out",
    )
    grad_normed = seq_scatter(gpart, n_seq, 2, 9)
    grad_row_norm, grad_gmix = norm_pullback(grad_normed)
    grad_tokens = grad_row_norm + grad_resid

    ggains = lax.psum_scatter(
        jnp.stack([grad_gmix, grad_gmoe]), both, scatter_dimension=1, tiled=True
    )
    gw = gw.reshape(d_model, 2, cp)[:, :, :chans].reshape(d_model, 2 * chans).astype(bf16)
    gw = lax.psum_scatter(gw, "dp", scatter_dimension=0, tiled=True)
    gw = lax.all_to_all(gw.reshape(n_seq, rows_in, 2 * chans), "seq", 0, 0, tiled=True)
    gw = gw.reshape(n_seq, rows_in, 2, n_dp, cpd).transpose(1, 2, 3, 0, 4)
    grad_win = gw.reshape(rows_in, 2 * n_dp * n_seq * cpd).astype(f32)
    gpack = jnp.concatenate(
        [gwx[:, :n_small], gwdt[:, :rank], gcw[:4].T, (ga * a_neg).T, gvecs[:2].T], axis=1
    )[:chans]
    gpack = lax.psum_scatter(gpack, "dp", scatter_dimension=0, tiled=True)
    grad_wout = lax.psum_scatter(
        gwout[:chans].astype(bf16), "dp", scatter_dimension=0, tiled=True
    ).astype(f32)
    edges = [p - d_model for p in places[1:]]
    gwx_m, gwdt_m, gconv_m, galog_m, gbias_m, gskip_m = [
        gpack[:, a:b] for a, b in zip(edges[:-1], edges[1:])
    ]
    return (
        result, grad_tokens, ggains[0], grad_win, gconv_m, gwx_m, gwdt_m, gbias_m[:, 0], galog_m,
        gskip_m[:, 0], grad_wout, ggains[1], grad_up[None], grad_down[None],
    )


def solution(mesh):
    row2, row1 = P(("dp", "seq"), None), P(("dp", "seq"))
    mats = P("dp", "seq", None)
    return jax.shard_map(
        on_device,
        mesh=mesh,
        in_specs=(
            row2, row2, row2, row1, row2, row2, row2, row2, row1, row2, row1, row2, row1, mats, mats
        ),
        out_specs=(
            row2, row2, row1, row2, row2, row2, row2, row1, row2, row1, row2, row1, mats, mats
        ),
        check_vma=False,
    )
```

```python
from functools import partial

import jax
import jax.numpy as jnp
from jax import lax
from jax.experimental import pallas as pl
from jax.experimental.pallas import tpu as pltpu
from jax.sharding import PartitionSpec as P

NS = 16
LN2 = 0.6931471805599453
LOG2E = 1.4426950408889634
eps = 1e-05
f32 = jnp.float32
bf16 = jnp.bfloat16

NN = (((1,), (0,)), ((), ()))
NT = (((1,), (1,)), ((), ()))
TN = (((0,), (0,)), ((), ()))


def mm(left, right, dims=NN):
    return lax.dot_general(left, right, dims, preferred_element_type=f32)


def up128(count):
    return -(-count // 128) * 128


def rms_norm(values, gain_vec):
    return values * lax.rsqrt(jnp.mean(values * values, axis=-1, keepdims=True) + eps) * gain_vec


def sigmoid(v):
    return 1.0 / (1.0 + jnp.exp(-v))


def softplus(v):
    return jnp.maximum(v, 0.0) + jnp.log1p(jnp.exp(-jnp.abs(v)))


def tree_step(first, second, by):
    row = lax.broadcasted_iota(jnp.int32, first.shape, 0)
    clear = (row & by) == 0
    return jnp.where(clear, first, second) + pltpu.roll(jnp.where(clear, second, first), by, 0)


def tree_push(stack, value, falling=False):
    level = 1
    while stack and stack[-1][0] == level:
        other = stack.pop()[1]
        value = tree_step(value, other, level) if falling else tree_step(other, value, level)
        level *= 2
    stack.append((level, value))


def turned(misc):
    return misc[...].astype(f32).T


def in_kernel(tok, gain, w, wx, misc, x_out, z_out, conv_out, small_out, norm_out, buf, mt):
    rows, cp = x_out.shape

    @pl.when(pl.program_id(0) == 0)
    def _():
        buf[0:8, :] = jnp.zeros((8, cp), f32)
        mt[...] = turned(misc)

    @pl.when(pl.program_id(0) > 0)
    def _():
        buf[0:8, :] = buf[rows : rows + 8, :]

    normed = rms_norm(tok[...].astype(f32), gain[0:1, :]).astype(bf16)
    norm_out[...] = normed
    prod = mm(normed, w[...])
    x_part = prod[:, :cp]
    x_out[...] = x_part
    z_out[...] = prod[:, cp:]
    buf[8 : 8 + rows, :] = x_part
    conv = x_part * mt[3:4, :]
    for k in range(3):
        conv = conv + buf[5 + k : 5 + k + rows, :] * mt[k : k + 1, :]
    conv_out[...] = conv
    small_out[...] = mm((conv * sigmoid(conv)).astype(bf16), wx[...]).astype(bf16)


def stage_step(k, n, steps):
    return steps - 1 - (n - 1 - k) * max(1, (steps - 2) // max(1, n - 1))


def scan_kernel(
    n_seq, steps, small, bct, wdt, misc, conv, z, wout, cot_own,
    dtp_out, h_out, ssm_out, gated_out, part_out, cot_all,
    delta_s, du_s, state, mt, a2, csem, *gsems,
):
    rows, cp = conv.shape
    line = Line(n_seq)
    step = pl.program_id(0)
    slots_of = Gather(
        line, lambda q, p: cot_all.at[q, p], lambda p: cot_own.at[p], cot_own.shape[0], gsems
    )
    own = pltpu.make_async_copy(cot_own, cot_all.at[line.me], csem)

    @pl.when(step == 0)
    def _():
        greet(line.neighbours())
        own.start()
        slots_of.stage(0)

    for k in range(1, line.n):
        pl.when(step == stage_step(k, line.n, steps))(lambda k=k: slots_of.stage(k))

    @pl.when(pl.program_id(0) == 0)
    def _():
        state[...] = jnp.zeros_like(state)
        mt[...] = turned(misc)
        a2[...] = -jnp.exp(mt[16:32, :]) * LOG2E

    dtp = mm(small[...], wdt[...], NT) + mt[8:9, :]
    dtp_out[...] = dtp
    delta = softplus(dtp)
    cv = conv[...]
    u = cv * sigmoid(cv)
    delta_s[...] = delta
    du_s[...] = delta * u

    def group(g, h):
        base = pl.multiple_of(g * 8, 8)
        bc = bct[g]
        stack = []
        for t in range(8):
            d = jnp.broadcast_to(delta_s[pl.ds(base + t, 1), :], (NS, cp))
            du = jnp.broadcast_to(du_s[pl.ds(base + t, 1), :], (NS, cp))
            h = jnp.exp2(d * a2[...]) * h + du * bc[:NS, t : t + 1]
            h_out[base + t] = h
            prod = h * bc[NS:, t : t + 1]
            tree_push(stack, prod[:8] + prod[8:])
        ssm_out[pl.ds(base, 8), :] = stack[0][1]
        return h

    state[...] = lax.fori_loop(0, rows // 8, group, state[...])
    zv = z[...]
    gated = (ssm_out[...] + mt[9:10, :] * u) * (zv * sigmoid(zv))
    low = gated.astype(bf16)
    gated_out[...] = low
    part_out[...] = mm(low, wout[...]).astype(part_out.dtype)

    @pl.when(step == steps - 1)
    def _():
        slots_of.finish()
        own.wait()


def back_kernel(
    n_seq, steps, gml, wout, gated, conv, z, ssm, dtp, hs, hlast, bct, small, wdt, misc,
    term, rank_out, gbct_out, gu_out, gz_out, gwout_out, gwdt, gmisc, sums_out,
    delta_s, du_s, gs_s, r1_s, r2_s, lam_s, mt, a2, gwout, ga, *scratch,
):
    rows, cp = conv.shape
    step = pl.program_id(0)
    last = steps - 1
    line = Line(n_seq)
    work = Collect(line, term, sums_out, scratch)

    @pl.when(step == 0)
    def _():
        greet(line.neighbours(), work.peers)
        work.open()

    for t in range(line.n):
        pl.when(step == t + 1)(lambda t=t: work.stage(t))

    @pl.when(step == 0)
    def _():
        lam_s[...] = jnp.zeros_like(lam_s)
        gwout[...] = jnp.zeros_like(gwout)
        gwdt[...] = jnp.zeros_like(gwdt)
        ga[...] = jnp.zeros_like(ga)
        gmisc[...] = jnp.zeros_like(gmisc)
        mt[...] = turned(misc)
        a2[...] = -jnp.exp(mt[16:32, :]) * LOG2E

    grad_mixed = gml[...]
    gg = mm(grad_mixed, wout[...], NT)
    gwout[...] += mm(gated[...], grad_mixed, TN)
    zv = z[...]
    sz = sigmoid(zv)
    cv = conv[...]
    u = cv * sigmoid(cv)
    skip = mt[9:10, :]
    gz_out[...] = (gg * (ssm[...] + skip * u) * (sz * (1.0 + zv * (1.0 - sz)))).astype(bf16)
    gs = gg * (zv * sz)
    delta = softplus(dtp[...])
    gs_s[...] = gs
    delta_s[...] = delta
    du_s[...] = delta * u
    lane = lax.broadcasted_iota(jnp.int32, (NS, 128), 1)
    keep_first = jnp.where(step == last, 0.0, 1.0)
    tiles = cp // 128

    def lane_fold(v):
        total = v[:, :128]
        for i in range(1, tiles):
            total = total + v[:, i * 128 : (i + 1) * 128]
        return jnp.sum(total, axis=1, keepdims=True)

    def group(k, carry):
        lamd, acc = carry
        g = rows // 8 - 1 - k
        base = pl.multiple_of(g * 8, 8)
        bc = bct[g]
        stack1, stack2 = [], []
        gb = jnp.zeros((NS, 128), f32)
        gc = jnp.zeros((NS, 128), f32)
        h = hs[base + 7]
        for t in range(7, -1, -1):
            d = jnp.broadcast_to(delta_s[pl.ds(base + t, 1), :], (NS, cp))
            du = jnp.broadcast_to(du_s[pl.ds(base + t, 1), :], (NS, cp))
            g_s = jnp.broadcast_to(gs_s[pl.ds(base + t, 1), :], (NS, cp))
            if t > 0:
                before = hs[base + t - 1]
            else:
                inside = hs[jnp.maximum(base - 1, 0)]
                before = jnp.where(g == 0, hlast[0] * keep_first, inside)
            lam = lamd + g_s * bc[NS:, t : t + 1]
            gc = jnp.where(lane == t, lane_fold(g_s * h), gc)
            gb = jnp.where(lane == t, lane_fold(lam * du), gb)
            lamd = jnp.exp2(d * a2[...]) * lam
            w = lamd * before
            acc = acc + w * d
            wa = w * a2[...]
            lb = lam * bc[:NS, t : t + 1]
            tree_push(stack1, wa[:8] + wa[8:], True)
            tree_push(stack2, lb[:8] + lb[8:], True)
            h = before
        r1_s[pl.ds(base, 8), :] = stack1[0][1]
        r2_s[pl.ds(base, 8), :] = stack2[0][1]
        gbct_out[g, :NS, :] = gb[:, :8]
        gbct_out[g, NS:, :] = gc[:, :8]
        return lamd, acc

    lamd, acc = lax.fori_loop(0, rows // 8, group, (lam_s[...], jnp.zeros((NS, cp), f32)))
    lam_s[...] = lamd
    ga[...] += acc
    r2 = r2_s[...]
    gu_out[...] = skip * gs + delta * r2
    gdelta = r1_s[...] * LN2 + u * r2
    gdtp = gdelta * sigmoid(dtp[...])
    gmisc[8:9, :] += jnp.sum(gdtp, axis=0, keepdims=True)
    gmisc[9:10, :] += jnp.sum(gs * u, axis=0, keepdims=True)
    low = gdtp.astype(bf16)
    gwdt[...] += mm(low, small[...], TN)
    rank_out[...] = mm(low, wdt[...])

    @pl.when(step == last)
    def _():
        gmisc[16:32, :] = ga[...] * (a2[...] * LN2)
        parts, cpd, _ = gwout_out.shape
        for p in range(parts):
            gwout_out[p] = gwout[p * cpd : (p + 1) * cpd, :].astype(bf16)
        work.finish()


def out_kernel(
    gsmall, wx, misc, conv, x, gu, gz, norm, w, gwdt, gmisc, part_out, gw_out, pack_out,
    buf, mt, gwx, gw, gm,
):
    rows, cp = conv.shape

    @pl.when(pl.program_id(0) == 0)
    def _():
        buf[rows : rows + 8, :] = jnp.zeros((8, cp), f32)
        gwx[...] = jnp.zeros_like(gwx)
        gw[...] = jnp.zeros_like(gw)
        gm[...] = jnp.zeros_like(gm)
        gm[8:32, :] = gmisc[8:32, :]
        mt[...] = turned(misc)

    @pl.when(pl.program_id(0) > 0)
    def _():
        buf[rows : rows + 8, :] = buf[0:8, :]

    gsl = gsmall[...]
    cv = conv[...]
    s = sigmoid(cv)
    gwx[...] += mm((cv * s).astype(bf16), gsl, TN)
    gconv = (gu[...] + mm(gsl, wx[...], NT)) * (s * (1.0 + cv * (1.0 - s)))
    buf[0:rows, :] = gconv
    xv = x[...]
    gx = gconv * mt[3:4, :]
    gm[3:4, :] += jnp.sum(gconv * xv, axis=0, keepdims=True)
    for k in range(3):
        moved = buf[3 - k : 3 - k + rows, :]
        gx = gx + moved * mt[k : k + 1, :]
        gm[k : k + 1, :] += jnp.sum(moved * xv, axis=0, keepdims=True)
    gp = jnp.concatenate([gx.astype(bf16), gz[...]], axis=1)
    part_out[...] = mm(gp, w[...], NT).astype(part_out.dtype)
    gw[...] += mm(norm[...], gp, TN)

    @pl.when(pl.program_id(0) == pl.num_programs(0) - 1)
    def _():
        parts, blocks, high, _ = gw_out.shape
        for b in range(parts * blocks):
            gw_out[b // blocks, b % blocks] = gw[b * high : (b + 1) * high, :].astype(bf16)
        flat = gm[...].T
        cpd = pack_out.shape[1]
        for p in range(parts):
            own = slice(p * cpd, (p + 1) * cpd)
            pack_out[p, :, 0:128] = gwx[own, :]
            pack_out[p, :, 128:256] = gwdt[own, :]
            pack_out[p, :, 256:384] = flat[own, :]


def chunked(kernel, steps, backward, ins, outs, scratch, name, number=None):
    def at(i):
        return steps - 1 - i if backward else i

    def spec(shape, rows):
        tail = (0,) * (len(shape) - 1)
        if rows is None:
            return pl.BlockSpec(memory_space=pl.ANY)
        if isinstance(rows, tuple):
            (block, column), = rows
            return pl.BlockSpec(block, lambda i: (0, column))
        if rows == 0:
            return pl.BlockSpec(shape, lambda i: (0,) + tail)
        if rows < 0:
            return pl.BlockSpec((1,) + shape[1:], lambda i: (jnp.maximum(at(i) * -rows - 1, 0),) + tail)
        return pl.BlockSpec((rows,) + shape[1:], lambda i: (at(i),) + tail)

    return pl.pallas_call(
        kernel,
        grid=(steps,),
        in_specs=[spec(a.shape, r) for a, r in ins],
        out_specs=[spec(s.shape, r) for s, r in outs],
        out_shape=[s for s, _ in outs],
        scratch_shapes=scratch,
        name=name,
        compiler_params=pltpu.CompilerParams(
            dimension_semantics=("arbitrary",), vmem_limit_bytes=60 * 1024 * 1024,
            collective_id=number, has_side_effects=number is not None,
        ),
    )(*[a for a, _ in ins])


MESH = pl.DeviceIdType.MESH


def remote(src, dst, send, recv, **where):
    return pltpu.make_async_remote_copy(
        src_ref=src, dst_ref=dst, send_sem=send, recv_sem=recv, device_id=where, device_id_type=MESH
    )


class Line:
    def __init__(self, n_seq):
        assert n_seq % 2 == 0
        self.n = n_seq // 2
        self.n_seq = n_seq
        self.me = lax.axis_index("seq")
        self.o, self.i = self.me // 2, self.me % 2

    def at(self, o, i):
        return o * 2 + i

    def neighbours(self):
        return [
            (None, self.at(self.o, 1 - self.i)),
            (self.o > 0, self.at(self.o - 1, self.i)),
            (self.o < self.n - 1, self.at(self.o + 1, self.i)),
        ]

    def order(self, t):
        table = [
            sorted(range(self.n), key=lambda q, o=o: (-abs(q - o), -q))[t] for o in range(self.n)
        ]
        place = jnp.int32(0)
        for o in range(self.n):
            place = place + jnp.where(self.o == o, table[o], 0)
        return place


def when(condition, action):
    if condition is None:
        action()
    else:
        pl.when(condition)(action)


def greet(peers, extra=()):
    barrier = pltpu.get_barrier_semaphore()
    count = jnp.int32(0)
    for condition, place in peers:
        when(
            condition,
            lambda place=place: pl.semaphore_signal(
                barrier, inc=1, device_id={"seq": place}, device_id_type=MESH
            ),
        )
        count = count + (1 if condition is None else jnp.where(condition, 1, 0))
    for place in extra:
        pl.semaphore_signal(barrier, inc=1, device_id={"dp": place}, device_id_type=MESH)
        count = count + 1
    pl.semaphore_wait(barrier, count)


def gather_sems(n, pieces):
    dma = pltpu.SemaphoreType.DMA
    return [dma((n, pieces)), dma((pieces,)), dma((n, pieces)), dma((n, pieces)), dma((n, pieces))]


class Gather:
    def __init__(self, line, at, own, pieces, sems):
        self.line, self.at, self.own, self.pieces, self.sems = line, at, own, pieces, sems

    def copy(self, src, q, p, send, recv, place):
        return remote(src, self.at(self.line.at(q, self.line.i), p), send, recv, seq=place)

    def up(self, src, q, p):
        zs, _, zr, _, _ = self.sems
        return self.copy(src, q, p, zs.at[q, p], zr.at[q, p], self.line.at(self.line.o + 1, self.line.i))

    def down(self, src, q, p, own):
        zs, zd, zr, _, _ = self.sems
        send = zd.at[p] if own else zs.at[q, p]
        return self.copy(src, q, p, send, zr.at[q, p], self.line.at(self.line.o - 1, self.line.i))

    def over(self, src, q, p):
        _, _, _, ys, yr = self.sems
        return self.copy(src, q, p, ys.at[q, p], yr.at[q, p], self.line.at(self.line.o, 1 - self.line.i))

    def each(self, k, act, arrive=None):
        line, o, n = self.line, self.line.o, self.line.n
        for p in range(self.pieces):
            if k == 0:
                src = self.own(p)
                if arrive is not None:
                    arrive(p)
                pl.when(o < n - 1)(lambda src=src, p=p: act(self.up(src, o, p)))
                pl.when(o > 0)(lambda src=src, p=p: act(self.down(src, o, p, True)))
                act(self.over(src, o, p))
                continue

            def below(p=p):
                q = o - k
                src = self.at(line.at(q, line.i), p)
                if arrive is not None:
                    arrive(self.up(src, q, p))
                pl.when(o < n - 1)(lambda: act(self.up(src, q, p)))
                act(self.over(src, q, p))

            def above(p=p):
                q = o + k
                src = self.at(line.at(q, line.i), p)
                if arrive is not None:
                    arrive(self.up(src, q, p))
                pl.when(o > 0)(lambda: act(self.down(src, q, p, False)))
                act(self.over(src, q, p))

            pl.when(o >= k)(below)
            pl.when(o + k <= n - 1)(above)

    def stage(self, k, ready=None):
        arrive = ready if k == 0 else (lambda copy: copy.wait_recv())
        self.each(k, lambda copy: copy.start(), arrive)

    def finish(self):
        line = self.line
        for q in range(line.n):
            for p in range(self.pieces):
                here = self.at(line.at(q, 1 - line.i), p)
                self.over(here, q, p).wait_recv()
        for k in range(line.n):
            self.each(k, lambda copy: copy.wait_send())

    def run(self, ready=None):
        for k in range(self.line.n):
            self.stage(k, ready)
        self.finish()


def gather_kernel(n_seq, x, out, lsem, *sems):
    line = Line(n_seq)
    greet(line.neighbours())
    keep = pltpu.make_async_copy(x, out.at[line.me], lsem)
    keep.start()
    Gather(line, lambda q, p: out.at[q, p], lambda p: x.at[p], x.shape[0], sems).run()
    keep.wait()


def seq_gather(x, n_seq, pieces, number):
    rows, width = x.shape
    out = pl.pallas_call(
        partial(gather_kernel, n_seq),
        in_specs=[pl.BlockSpec(memory_space=pl.ANY)],
        out_specs=pl.BlockSpec(memory_space=pl.ANY),
        out_shape=jax.ShapeDtypeStruct((n_seq, pieces, rows // pieces, width), x.dtype),
        scratch_shapes=[pltpu.SemaphoreType.DMA] + gather_sems(n_seq // 2, pieces),
        compiler_params=pltpu.CompilerParams(collective_id=number, has_side_effects=True),
        name="seq_gather",
    )(x.reshape(pieces, rows // pieces, width))
    return out.reshape(n_seq * rows, width)


def dispatch_kernel(n_seq, n_dp, x, out, lsem, dps, dpr, *sems):
    line = Line(n_seq)
    mine = lax.axis_index("dp")
    peers = [lax.rem(mine + r, n_dp) for r in range(1, n_dp)]
    greet(line.neighbours(), peers)
    copies = []
    for r, peer in enumerate(peers):
        copy = remote(x.at[peer], out.at[line.me, mine], dps.at[r], dpr.at[r], dp=peer)
        copy.start()
        copies.append(copy)
    keep = pltpu.make_async_copy(x.at[mine], out.at[line.me, mine], lsem)
    keep.start()

    def ready(r):
        if r == 0:
            keep.wait()
        else:
            source = out.at[line.me, lax.rem(mine + n_dp - r, n_dp)]
            remote(source, source, dps.at[r - 1], dpr.at[r - 1], dp=peers[r - 1]).wait_recv()

    at = rolled(out, mine, n_dp)
    Gather(line, at, lambda r: at(line.me, r), n_dp, sems).run(ready)
    for copy in copies:
        copy.wait_send()


def rolled(out, mine, n_dp):
    return lambda q, r: out.at[q, lax.rem(mine + n_dp - r, n_dp)]


def dispatch_call(x, n_seq, number):
    n_dp, rows, width = x.shape
    dma = pltpu.SemaphoreType.DMA
    return pl.pallas_call(
        partial(dispatch_kernel, n_seq, n_dp),
        in_specs=[pl.BlockSpec(memory_space=pl.ANY)],
        out_specs=pl.BlockSpec(memory_space=pl.ANY),
        out_shape=jax.ShapeDtypeStruct((n_seq, n_dp, rows, width), x.dtype),
        scratch_shapes=[dma, dma((n_dp - 1,)), dma((n_dp - 1,))] + gather_sems(n_seq // 2, n_dp),
        compiler_params=pltpu.CompilerParams(collective_id=number, has_side_effects=True),
        name="dispatch",
    )(x)


def scatter_scratch(n, pieces, rows, width):
    dma = pltpu.SemaphoreType.DMA
    return [
        pltpu.VMEM((n, pieces, rows, width), bf16),
        pltpu.VMEM((n, pieces, rows, width), bf16),
        pltpu.VMEM((n + 1, pieces, rows, width), bf16),
        dma((n, pieces)), dma((n, pieces)), dma((n, pieces)), dma((n + 1, pieces)),
    ]


class Scatter:
    def __init__(self, line, at, pieces, scratch, final):
        self.line, self.at, self.pieces, self.final = line, at, pieces, final
        self.ybuf, self.zout, self.zin, self.ys, self.yr, self.zs, self.zr = scratch

    def over(self, t, p):
        q, line = self.line.order(t), self.line
        return remote(self.at(line.at(q, 1 - line.i), p), self.ybuf.at[q, p], self.ys.at[q, p],
                      self.yr.at[q, p], seq=line.at(line.o, 1 - line.i))

    def along(self, t, p):
        q, line = self.line.order(t), self.line
        up = q > line.o
        to = jnp.where(up, line.o + 1, line.o - 1)
        slot = jnp.where(jnp.logical_and(q == to, jnp.logical_not(up)), line.n, q)
        return remote(self.zout.at[q, p], self.zin.at[slot, p], self.zs.at[q, p], self.zr.at[slot, p],
                      seq=line.at(to, line.i))

    def arrived(self, k, p):
        here, line = self.zin.at[k, p], self.line
        remote(here, here, self.zs.at[0, p], self.zr.at[k, p],
               seq=line.at(line.o, 1 - line.i)).wait_recv()

    def open(self):
        for t in range(self.line.n):
            for p in self.pieces:
                self.over(t, p).start()

    def stage(self, t):
        line = self.line
        o, n = line.o, line.n
        q = line.order(t)
        for p in self.pieces:
            self.over(t, p).wait_recv()
            value = self.at(line.at(q, line.i), p)[...].astype(f32) + self.ybuf[q, p].astype(f32)
            if t < n - 1:
                fed = jnp.where(q > o, o > 0, o < n - 1)

                def with_feed(value=value, p=p):
                    self.arrived(q, p)
                    self.zout[q, p] = (value + self.zin[q, p].astype(f32)).astype(bf16)

                def without(value=value, p=p):
                    self.zout[q, p] = value.astype(bf16)

                pl.when(fed)(with_feed)
                pl.when(jnp.logical_not(fed))(without)
                self.along(t, p).start()
            else:
                below, above = o > 0, o < n - 1
                pl.when(below)(lambda p=p: self.arrived(o, p))
                pl.when(above)(lambda p=p: self.arrived(n, p))
                value = value + jnp.where(below, self.zin[o, p].astype(f32), 0.0)
                value = value + jnp.where(above, self.zin[n, p].astype(f32), 0.0)
                self.final(p, value)

    def finish(self):
        for t in range(self.line.n):
            for p in self.pieces:
                self.over(t, p).wait_send()
                if t < self.line.n - 1:
                    self.along(t, p).wait_send()

    def run(self):
        self.open()
        for t in range(self.line.n):
            self.stage(t)
        self.finish()


def scatter_kernel(n_seq, term, out, *scratch):
    line = Line(n_seq)
    greet(line.neighbours())

    def final(p, value):
        out[p] = value

    Scatter(line, lambda q, p: term.at[q, p], range(term.shape[1]), scratch, final).run()


def seq_scatter(x, n_seq, pieces, number):
    rows, width = x.shape[0] // n_seq, x.shape[1]
    part = rows // pieces
    vmem = pl.BlockSpec(memory_space=pltpu.VMEM)
    out = pl.pallas_call(
        partial(scatter_kernel, n_seq),
        in_specs=[vmem],
        out_specs=vmem,
        out_shape=jax.ShapeDtypeStruct((pieces, part, width), f32),
        scratch_shapes=scatter_scratch(n_seq // 2, pieces, part, width),
        compiler_params=pltpu.CompilerParams(
            collective_id=number, has_side_effects=True, vmem_limit_bytes=60 * 1024 * 1024
        ),
        name="seq_scatter",
    )(x.reshape(n_seq, pieces, part, width))
    return out.reshape(rows, width)


class Collect:
    def __init__(self, line, term, out, scratch):
        self.line, self.term, self.out = line, term, out
        self.sumbuf, self.lsem, self.dps, self.dpr = scratch[:4]
        self.n_dp = term.shape[1]
        self.mine = lax.axis_index("dp")
        self.peers = [lax.rem(self.mine + r, self.n_dp) for r in range(1, self.n_dp)]

        def at(q, r):
            return term.at[q, lax.rem(self.mine + r, self.n_dp)]

        def final(r, value):
            self.sumbuf[r] = value.astype(bf16)
            self.back(r).start()

        pieces = list(range(1, self.n_dp)) + [0]
        self.scatter = Scatter(line, at, pieces, scratch[4:], final)
        self.open, self.stage = self.scatter.open, self.scatter.stage

    def back(self, r):
        if r == 0:
            return pltpu.make_async_copy(self.sumbuf.at[0], self.out.at[self.mine], self.lsem)
        return remote(self.sumbuf.at[r], self.out.at[self.mine], self.dps.at[r - 1], self.dpr.at[r - 1],
                      dp=self.peers[r - 1])

    def finish(self):
        self.scatter.finish()
        for r in range(1, self.n_dp):
            here = self.out.at[lax.rem(self.mine + self.n_dp - r, self.n_dp)]
            remote(here, here, self.dps.at[r - 1], self.dpr.at[r - 1],
                   dp=self.peers[r - 1]).wait_recv()
            self.back(r).wait_send()
        self.back(0).wait()


def collect_scratch(n_seq, n_dp, rows, width):
    dma = pltpu.SemaphoreType.DMA
    return [pltpu.VMEM((n_dp, rows, width), bf16), dma, dma((n_dp - 1,)), dma((n_dp - 1,))] + (
        scatter_scratch(n_seq // 2, n_dp, rows, width)
    )


def collect_kernel(n_seq, term, out, *scratch):
    line = Line(n_seq)
    work = Collect(line, term, out, scratch)
    greet(line.neighbours(), work.peers)
    work.open()
    for t in range(line.n):
        work.stage(t)
    work.finish()


def collect_call(x, n_seq, number):
    _, n_dp, rows, width = x.shape
    vmem = pl.BlockSpec(memory_space=pltpu.VMEM)
    return pl.pallas_call(
        partial(collect_kernel, n_seq),
        in_specs=[vmem],
        out_specs=vmem,
        out_shape=jax.ShapeDtypeStruct((n_dp, rows, width), bf16),
        scratch_shapes=collect_scratch(n_seq, n_dp, rows, width),
        compiler_params=pltpu.CompilerParams(
            collective_id=number, has_side_effects=True, vmem_limit_bytes=60 * 1024 * 1024
        ),
        name="collect",
    )(x)


def sum_kernel(n_seq, x, out, inbox, total, lsem, s1, r1, s2, r2):
    me = lax.axis_index("seq")
    peers = [lax.rem(me + r, n_seq) for r in range(1, n_seq)]
    greet([(None, q) for q in peers])
    copies = []
    for r, q in enumerate(peers):
        copy = remote(x.at[q], inbox.at[r], s1.at[r], r1.at[r], seq=q)
        copy.start()
        copies.append(copy)
    value = x[me].astype(f32)
    for r, q in enumerate(peers):
        remote(inbox.at[r], inbox.at[r], s1.at[r], r1.at[r], seq=q).wait_recv()
        value = value + inbox[r].astype(f32)
    total[...] = value.astype(total.dtype)
    for r, q in enumerate(peers):
        copy = remote(total, out.at[me], s2.at[r], r2.at[r], seq=q)
        copy.start()
        copies.append(copy)
    keep = pltpu.make_async_copy(total, out.at[me], lsem)
    keep.start()
    for r, q in enumerate(peers):
        here = out.at[lax.rem(me + n_seq - 1 - r, n_seq)]
        remote(here, here, s2.at[r], r2.at[r], seq=q).wait_recv()
    keep.wait()
    for copy in copies:
        copy.wait_send()


def seq_sum(x, n_seq, number):
    rows, width = x.shape[0] // n_seq, x.shape[1]
    dma = pltpu.SemaphoreType.DMA
    vmem = pl.BlockSpec(memory_space=pltpu.VMEM)
    out = pl.pallas_call(
        partial(sum_kernel, n_seq),
        in_specs=[vmem],
        out_specs=vmem,
        out_shape=jax.ShapeDtypeStruct((n_seq, rows, width), x.dtype),
        scratch_shapes=[pltpu.VMEM((n_seq - 1, rows, width), x.dtype), pltpu.VMEM((rows, width), x.dtype),
                        dma] + [dma((n_seq - 1,)) for _ in range(4)],
        compiler_params=pltpu.CompilerParams(
            collective_id=number, has_side_effects=True, vmem_limit_bytes=60 * 1024 * 1024
        ),
        name="seq_sum",
    )(x.reshape(n_seq, rows, width))
    return out.reshape(n_seq * rows, width)


def all_peers(n_seq):
    me = lax.axis_index("seq")
    return [lax.rem(me + r, n_seq) for r in range(1, n_seq)]


def dp_peers():
    mine = lax.axis_index("dp")
    other = mine + 1 - 2 * lax.rem(mine, 2)
    return mine, other, lax.rem(mine + 2, 4), lax.rem(other + 2, 4)


class Spread:
    def __init__(self, out, sems):
        self.out, (self.s, self.r) = out, sems
        self.mine, self.core, self.far, self.rest = dp_peers()
        self.sent = []

    def push(self, src, place, k, peer):
        copy = remote(src, self.out.at[place], self.s.at[k], self.r.at[k], dp=peer)
        copy.start()
        self.sent.append(copy)

    def wait(self, place, k):
        here = self.out.at[place]
        remote(here, here, self.s.at[k], self.r.at[k], dp=self.core).wait_recv()

    def start(self, src):
        self.push(src, self.mine, 1, self.far)
        self.push(src, self.mine, 0, self.core)

    def forward(self):
        self.wait(self.far, 1)
        self.push(self.out.at[self.far], self.far, 2, self.core)

    def finish(self):
        self.wait(self.core, 0)
        self.wait(self.rest, 2)
        for copy in self.sent:
            copy.wait_send()


def start_kernel(
    n_seq, tok, w_in, wout, side, gains, route, cot,
    xg, w_all, wout_all, side_all, gain_all, cot_own, pick_out,
    wst, gbox, zero_w, zero_s, cst, lsem, tsem, csem, cds, cdr, *sems,
):
    gsems, (a2s, a2r, gs2, gr2), dsems = sems[:5], sems[5:9], sems[9:]
    line = Line(n_seq)
    me = line.me
    peers = all_peers(n_seq)
    mine, core, far, rest = dp_peers()
    greet([(None, q) for q in peers], [core, far, rest])
    keep = pltpu.make_async_copy(tok, xg.at[me], tsem)
    keep.start()
    tokens_of = Gather(line, lambda q, p: xg.at[q, p], lambda p: tok.at[p], tok.shape[0], gsems)
    tokens_of.stage(0)
    locals_ = []

    def local(src, dst, k):
        copy = pltpu.make_async_copy(src, dst, lsem.at[k])
        copy.start()
        locals_.append(copy)

    gain_dp = Spread(gbox, dsems[0:2])
    gbox[mine] = gains[...]
    gain_dp.start(gains)
    w_dp = Spread(w_all, dsems[2:4])
    wout_dp = Spread(wout_all, dsems[4:6])
    side_dp = Spread(side_all, dsems[6:8])
    side_dp.start(side)
    wout_dp.start(wout)
    local(wout, wout_all.at[mine], 0)
    local(side, side_all.at[mine], 1)
    zero_w[...] = jnp.zeros_like(zero_w)
    zero_s[...] = jnp.zeros_like(zero_s)

    here = route.shape[0]
    n_dp, slots, _ = cot_own.shape
    expert = lax.broadcasted_iota(jnp.int32, (here, n_dp), 1)
    onehot = jnp.where(route[...] == expert, 1.0, 0.0)
    earlier = lax.broadcasted_iota(jnp.int32, (here, here), 1) < lax.broadcasted_iota(
        jnp.int32, (here, here), 0
    )
    before = mm(jnp.where(earlier, 1.0, 0.0).astype(bf16), onehot.astype(bf16))
    index = jnp.sum(before * onehot, axis=1, keepdims=True)
    target = route[...] * slots + index.astype(jnp.int32)
    slot = lax.broadcasted_iota(jnp.int32, (here, n_dp * slots), 1)
    pick = jnp.where(target == slot, 1.0, 0.0).astype(bf16)
    pick_out[...] = pick
    for e in range(n_dp):
        cst[e] = mm(pick[:, e * slots : (e + 1) * slots], cot[...], TN).astype(bf16)
    copies = []
    for k, peer in enumerate((core, far, rest)):
        copy = remote(cst.at[peer], cot_own.at[mine], cds.at[k], cdr.at[k], dp=peer)
        copy.start()
        copies.append(copy)
    keep_cot = pltpu.make_async_copy(cst.at[mine], cot_own.at[mine], csem)
    keep_cot.start()

    high, wide = w_in.shape
    cpd = wide // (2 * 4 * n_seq)
    half = wst.shape[2] // 2
    values = w_in[...].astype(f32)
    for q in range(n_seq):
        for side_of in range(2):
            first = side_of * 4 * n_seq
            parts = [
                values[:, (first + p * n_seq + q) * cpd : (first + p * n_seq + q + 1) * cpd]
                for p in range(4)
            ]
            if half > 4 * cpd:
                parts.append(jnp.zeros((high, half - 4 * cpd), f32))
            wst[q, :, side_of * half : (side_of + 1) * half] = jnp.concatenate(
                parts, axis=1
            ).astype(bf16)
    for r, q in enumerate(peers):
        copy = remote(wst.at[q], w_all.at[mine, me], a2s.at[r], a2r.at[r], seq=q)
        copy.start()
        copies.append(copy)
    local(wst.at[me], w_all.at[mine, me], 2)
    extra = wout_all.shape[0] - 4
    for k in range(extra):
        local(zero_w, wout_all.at[4 + k], 3 + 2 * k)
        local(zero_s, side_all.at[4 + k], 4 + 2 * k)
    gain_dp.forward()
    gain_dp.finish()
    for r, q in enumerate(peers):
        copy = remote(gbox, gain_all.at[me], gs2.at[r], gr2.at[r], seq=q)
        copy.start()
        copies.append(copy)
    gain_all[me] = gbox[...]
    tokens_of.stage(1)
    for r, q in enumerate(peers):
        here = w_all.at[mine, lax.rem(me + n_seq - 1 - r, n_seq)]
        remote(here, here, a2s.at[r], a2r.at[r], seq=q).wait_recv()
    for copy in locals_:
        copy.wait()
    w_dp.start(w_all.at[mine])
    if line.n > 2:
        tokens_of.stage(2)
    side_dp.forward()
    wout_dp.forward()
    for k in range(3, line.n):
        tokens_of.stage(k)
    w_dp.forward()
    tokens_of.finish()
    side_dp.finish()
    wout_dp.finish()
    for r, q in enumerate(peers):
        here = gain_all.at[lax.rem(me + n_seq - 1 - r, n_seq)]
        remote(here, here, gs2.at[r], gr2.at[r], seq=q).wait_recv()
    for k, peer in enumerate((core, far, rest)):
        remote(cot_own.at[peer], cot_own.at[peer], cds.at[k], cdr.at[k], dp=peer).wait_recv()
    keep_cot.wait()
    keep.wait()
    w_dp.finish()
    for copy in copies:
        copy.wait_send()


def start_call(tokens, w_in, w_out, side, gains, route, cot, slots, n_seq, cp, number):
    here, d_model = tokens.shape
    high, _ = w_in.shape
    cpd, n_side = side.shape
    extra = -(-cp // cpd) - 4
    dma = pltpu.SemaphoreType.DMA
    anyw, vmem = pl.BlockSpec(memory_space=pl.ANY), pl.BlockSpec(memory_space=pltpu.VMEM)
    sds = jax.ShapeDtypeStruct
    return pl.pallas_call(
        partial(start_kernel, n_seq),
        in_specs=[anyw, vmem, anyw, anyw, vmem, vmem, vmem],
        out_specs=[anyw, anyw, anyw, anyw, vmem, anyw, vmem],
        out_shape=[
            sds((n_seq, 2, here // 2, d_model), bf16),
            sds((4, n_seq, high, 2 * cp), bf16),
            sds((4 + extra, cpd, d_model), bf16),
            sds((4 + extra, cpd, n_side), bf16),
            sds((n_seq, 4, 8, 128), f32),
            sds((4, slots, d_model), bf16),
            sds((here, 4 * slots), bf16),
        ],
        scratch_shapes=[
            pltpu.VMEM((n_seq, high, 2 * cp), bf16), pltpu.VMEM((4, 8, 128), f32),
            pltpu.VMEM((cpd, d_model), bf16), pltpu.VMEM((cpd, n_side), bf16),
            pltpu.VMEM((4, slots, d_model), bf16),
            dma((3 + 2 * extra,)), dma, dma, dma((3,)), dma((3,)),
        ] + gather_sems(n_seq // 2, 2) + [dma((n_seq - 1,)) for _ in range(4)]
        + [dma((3,)) for _ in range(8)],
        compiler_params=pltpu.CompilerParams(
            collective_id=number, has_side_effects=True, vmem_limit_bytes=60 * 1024 * 1024
        ),
        name="startup",
    )(tokens.reshape(2, here // 2, d_model), w_in, w_out, side, gains, route, cot)


class Fold:
    def __init__(self, arr, box, send, sems):
        self.arr, self.box, self.send, (self.s, self.r) = arr, box, send, sems
        self.mine, self.core, self.far, self.rest = dp_peers()
        self.sent = []

    def push(self, src, k, peer):
        copy = remote(src, self.box.at[k], self.s.at[k], self.r.at[k], dp=peer)
        copy.start()
        self.sent.append(copy)

    def wait(self, k):
        remote(self.box.at[k], self.box.at[k], self.s.at[k], self.r.at[k], dp=self.core).wait_recv()

    def start(self):
        self.push(self.arr.at[self.rest], 1, self.core)
        self.push(self.arr.at[self.core], 0, self.core)

    def middle(self):
        self.wait(1)
        value = self.arr[self.far].astype(f32) + self.box[1].astype(f32)
        self.send[...] = value.astype(self.send.dtype)
        self.push(self.send, 2, self.far)

    def final(self):
        self.wait(0)
        self.wait(2)
        value = self.arr[self.mine].astype(f32) + self.box[0].astype(f32)
        return value + self.box[2].astype(f32)

    def done(self):
        for copy in self.sent:
            copy.wait_send()


def finish_kernel(
    n_seq, term, gwout, gw, pack, tok, gres, gains, ggmoe,
    gtok_out, gwout_out, pack_out, gwin_out, gain_out,
    gn, wsum, wbox, gst, gb1, gsum, gb2, o_box, o_send, w_box, w_send, p_box, p_send, lsem, *sems,
):
    scratch, (a2s, a2r, g1s, g1r, g2s, g2r), dsems = sems[:7], sems[7:13], sems[13:]
    line = Line(n_seq)
    me = line.me
    peers = all_peers(n_seq)
    mine, core, far, rest = dp_peers()
    dps = [core, far, rest]
    greet([(None, q) for q in peers], dps)
    f_w = Fold(gw, w_box, w_send, dsems[0:2])
    f_o = Fold(gwout, o_box, o_send, dsems[2:4])
    f_p = Fold(pack, p_box, p_send, dsems[4:6])
    for fold in (f_w, f_o, f_p):
        fold.start()

    def final(p, value):
        gn[p] = value

    sums = Scatter(line, lambda q, p: term.at[q, p], range(term.shape[1]), scratch, final)
    sums.open()
    for fold in (f_w, f_o, f_p):
        fold.middle()
    sums.stage(0)
    wsum[...] = f_w.final().astype(bf16)
    copies = []
    for r, q in enumerate(peers):
        copy = remote(wsum.at[q], wbox.at[me], a2s.at[r], a2r.at[r], seq=q)
        copy.start()
        copies.append(copy)
    keep = pltpu.make_async_copy(wsum.at[me], wbox.at[me], lsem)
    keep.start()
    if line.n > 1:
        sums.stage(1)
    gwout_out[...] = f_o.final()
    pack_out[...] = f_p.final()
    for t in range(2, line.n):
        sums.stage(t)
    sums.finish()

    v = tok[...].astype(f32)
    r_ = lax.rsqrt(jnp.mean(v * v, axis=-1, keepdims=True) + eps)
    gy = jnp.concatenate([gn[p] for p in range(gn.shape[0])], axis=0)
    gst[0:1, :] = jnp.sum(gy * (v * r_), axis=0, keepdims=True)
    gst[1:2, :] = ggmoe[...]
    gsends = []
    for k, peer in enumerate(dps):
        copy = remote(gst, gb1.at[k], g1s.at[k], g1r.at[k], dp=peer)
        copy.start()
        gsends.append(copy)
    gyg = gy * gains[0:1, :]
    inner = jnp.mean(gyg * v, axis=-1, keepdims=True)
    gtok_out[...] = gyg * r_ - v * (r_ * r_ * r_ * inner) + gres[...]
    total = gst[...]
    for k in range(3):
        remote(gb1.at[k], gb1.at[k], g1s.at[k], g1r.at[k], dp=core).wait_recv()
        total = total + gb1[k]
    gsum[...] = total
    for r, q in enumerate(peers):
        copy = remote(gsum, gb2.at[r], g2s.at[r], g2r.at[r], seq=q)
        copy.start()
        gsends.append(copy)

    keep.wait()
    for r, q in enumerate(peers):
        here = wbox.at[lax.rem(me + n_seq - 1 - r, n_seq)]
        remote(here, here, a2s.at[r], a2r.at[r], seq=q).wait_recv()
    wide = gwin_out.shape[1]
    cpd = wide // (2 * 4 * n_seq)
    half = wbox.shape[2] // 2
    for q in range(n_seq):
        block = wbox[q].astype(f32)
        for side_of in range(2):
            for p in range(4):
                at = (side_of * 4 * n_seq + p * n_seq + q) * cpd
                src = side_of * half + p * cpd
                gwin_out[:, at : at + cpd] = block[:, src : src + cpd]
    for r, q in enumerate(peers):
        remote(gb2.at[r], gb2.at[r], g2s.at[r], g2r.at[r], seq=q).wait_recv()
        total = total + gb2[r]
    gain_out[...] = total
    for fold in (f_w, f_o, f_p):
        fold.done()
    for copy in copies + gsends:
        copy.wait_send()


def finish_call(gpart, gwout, gw, pack, tokens, gres, gains, ggmoe, n_seq, number):
    here, d_model = tokens.shape
    _, _, high, wide = gw.shape
    _, cpd, n_side = pack.shape
    dma = pltpu.SemaphoreType.DMA
    vmem = pl.BlockSpec(memory_space=pltpu.VMEM)
    sds = jax.ShapeDtypeStruct
    mem = pltpu.VMEM
    return pl.pallas_call(
        partial(finish_kernel, n_seq),
        in_specs=[vmem] * 8,
        out_specs=[vmem] * 5,
        out_shape=[
            sds((here, d_model), f32), sds((cpd, d_model), f32), sds((cpd, n_side), f32),
            sds((high, 2 * 4 * n_seq * cpd), f32), sds((2, d_model), f32),
        ],
        scratch_shapes=[
            mem((2, here // 2, d_model), f32), mem((n_seq, high, wide), bf16), mem((n_seq, high, wide), bf16),
            mem((2, d_model), f32), mem((3, 2, d_model), f32), mem((2, d_model), f32),
            mem((n_seq - 1, 2, d_model), f32),
            mem((3, cpd, d_model), bf16), mem((cpd, d_model), bf16),
            mem((3, n_seq, high, wide), bf16), mem((n_seq, high, wide), bf16),
            mem((3, cpd, n_side), f32), mem((cpd, n_side), f32), dma,
        ] + scatter_scratch(n_seq // 2, 2, here // 2, d_model)
        + [dma((n_seq - 1,)), dma((n_seq - 1,)), dma((3,)), dma((3,)), dma((n_seq - 1,)), dma((n_seq - 1,))]
        + [dma((3,)) for _ in range(6)],
        compiler_params=pltpu.CompilerParams(
            collective_id=number, has_side_effects=True, vmem_limit_bytes=62 * 1024 * 1024
        ),
        name="finish",
    )(gpart.reshape(n_seq, 2, here // 2, d_model), gwout, gw, pack, tokens, gres, gains, ggmoe)


def on_device(
    tokens, route, cotangent, gain_mix, w_in, conv_w, w_x, w_dt, dt_bias, a_log, d_skip, w_out,
    gain_moe, w_up, w_down,
):
    n_seq, n_dp = lax.axis_size("seq"), lax.axis_size("dp")
    here, d_model = tokens.shape
    cpd = conv_w.shape[0]
    chans = cpd * n_dp
    cp = up128(chans)
    rank = w_dt.shape[1]
    n_small = w_x.shape[1]
    sp = up128(n_small)
    tall = here * n_seq
    rows_in = w_in.shape[0]
    experts, slots = n_dp, 40

    gap = jnp.zeros((cpd, 128), bf16)
    side = jnp.concatenate(
        [w_x, gap[:, n_small:], w_dt, gap[:, rank:], conv_w, gap[:, 4:8], dt_bias[:, None],
         d_skip[:, None], gap[:, 10:16], a_log, gap[:, 32:]], axis=1,
    )
    gains_in = jnp.pad(jnp.stack([gain_mix, gain_moe]).astype(f32), ((0, 6), (0, 128 - gain_mix.shape[0])))
    xg, w_all, wout_all, side_all, gain_all, cot_own, pick = start_call(
        tokens, w_in, w_out, side, gains_in, route, cotangent, slots, n_seq, cp, 0
    )
    toks = xg.reshape(tall, d_model)
    w_mine = w_all.reshape(n_dp * n_seq * rows_in, 2 * cp)
    wout_m = wout_all.reshape(-1, d_model)
    side_m = side_all.reshape(-1, 384)
    gains = gain_all[:, :, :2, : gain_mix.shape[0]].transpose(2, 1, 0, 3).reshape(2, d_model)
    wout_spec = (((cp, d_model), 0),)
    wx_spec, wdt_spec, misc_spec = [(((cp, 128), k),) for k in range(3)]

    row_values = tokens.astype(f32)
    tb = 128
    steps = tall // tb
    sds = jax.ShapeDtypeStruct
    wide = sds((tall, cp), f32)
    vec = pltpu.VMEM((tb, cp), f32)
    turned_misc = pltpu.VMEM((128, cp), f32)
    by_state = pltpu.VMEM((NS, cp), f32)
    x, z, conv, small, normed = chunked(
        in_kernel, steps, False,
        [(toks, tb), (gains, 0), (w_mine, 0), (side_m, wx_spec), (side_m, misc_spec)],
        [(wide, tb), (wide, tb), (wide, tb), (sds((tall, sp), bf16), tb), (sds((tall, d_model), bf16), tb)],
        [pltpu.VMEM((tb + 8, cp), f32), turned_misc], "mix_in",
    )
    small = seq_sum(small, n_seq, 1)
    bct = small[:, rank:n_small].astype(f32).reshape(tall // 8, 8, 2 * NS).transpose(0, 2, 1)
    dtp, hs, ssm, gated, part, grad_slots = chunked(
        partial(scan_kernel, n_seq, steps), steps, False,
        [(small, tb), (bct, tb // 8), (side_m, wdt_spec), (side_m, misc_spec), (conv, tb), (z, tb),
         (wout_m, wout_spec), (cot_own, None)],
        [(wide, tb), (sds((tall, NS, cp), f32), tb), (wide, tb), (sds((tall, cp), bf16), tb),
         (sds((tall, d_model), bf16), tb), (sds((n_seq, n_dp, slots, d_model), bf16), None)],
        [vec, vec, by_state, turned_misc, by_state, pltpu.SemaphoreType.DMA]
        + gather_sems(n_seq // 2, n_dp),
        "scan_forward", 3,
    )
    grad_slots = grad_slots.reshape(n_seq * n_dp * slots, d_model)
    mixer_out = seq_scatter(part, n_seq, 2, 2)
    resid = row_values + mixer_out

    normed2, norm2_pullback = jax.vjp(rms_norm, resid, gains[1])
    moe_in = normed2.astype(bf16)
    def dispatch(values, number):
        send = mm(pick, values, TN).astype(bf16).reshape(n_dp, slots, d_model)
        return dispatch_call(send, n_seq, number).reshape(n_seq * n_dp * slots, d_model)

    def returned(sums):
        return mm(pick, sums.reshape(n_dp * slots, d_model))

    shape4 = (n_seq, n_dp, slots, d_model)
    up, down = w_up[0], w_down[0]
    grad_hidden = mm(grad_slots, down, NT)
    slot_rows = dispatch(moe_in, 4)
    pre_act = mm(slot_rows, up, NT)
    hidden_f, gelu_pullback = jax.vjp(partial(jax.nn.gelu, approximate=False), pre_act)
    hidden = hidden_f.astype(bf16)
    grad_pre = gelu_pullback(grad_hidden)[0].astype(bf16)
    grad_moe_in = returned(collect_call(mm(grad_pre, up).astype(bf16).reshape(shape4), n_seq, 5))
    expert_terms = mm(hidden, down).astype(bf16).reshape(shape4)
    grad_down = mm(hidden, grad_slots, TN)
    grad_up = mm(grad_pre, slot_rows, TN)

    grad_resid, grad_gmoe = norm2_pullback(grad_moe_in)
    grad_resid = grad_resid + cotangent.astype(f32)
    gml = seq_gather(grad_resid.astype(bf16), n_seq, 2, 7)
    grad_rank, gbct, gu, gz, gwout, gwdt, gmisc, expert_out = chunked(
        partial(back_kernel, n_seq, steps), steps, True,
        [(gml, tb), (wout_m, wout_spec), (gated, tb), (conv, tb), (z, tb), (ssm, tb), (dtp, tb), (hs, tb),
         (hs, -tb), (bct, tb // 8), (small, tb), (side_m, wdt_spec), (side_m, misc_spec),
         (expert_terms, 0)],
        [(sds((tall, sp), f32), tb), (sds((tall // 8, 2 * NS, 8), f32), tb // 8), (wide, tb),
         (sds((tall, cp), bf16), tb), (sds((n_dp, cpd, d_model), bf16), 0), (sds((cp, sp), f32), 0),
         (sds((32, cp), f32), 0), (sds((n_dp, slots, d_model), bf16), None)],
        [vec] * 5 + [by_state, turned_misc, by_state, pltpu.VMEM((cp, d_model), f32), by_state]
        + collect_scratch(n_seq, n_dp, slots, d_model),
        "scan_backward", 6,
    )
    result = (resid + returned(expert_out)).astype(bf16)
    grad_bc = gbct.transpose(0, 2, 1).reshape(tall, 2 * NS)
    gsmall = jnp.concatenate([grad_rank[:, :rank], grad_bc], axis=1)
    gsmall = seq_sum(jnp.pad(gsmall, ((0, 0), (0, sp - n_small))).astype(bf16), n_seq, 8)
    gpart, gw, gpack = chunked(
        out_kernel, steps, True,
        [(gsmall, tb), (side_m, wx_spec), (side_m, misc_spec), (conv, tb), (x, tb), (gu, tb), (gz, tb),
         (normed, tb), (w_mine, 0), (gwdt, 0), (gmisc, 0)],
        [(sds((tall, d_model), bf16), tb), (sds((n_dp, n_seq, rows_in, 2 * cp), bf16), 0),
         (sds((n_dp, cpd, 384), f32), 0)],
        [pltpu.VMEM((tb + 8, cp), f32), turned_misc, pltpu.VMEM((cp, sp), f32),
         pltpu.VMEM((d_model, 2 * cp), f32), turned_misc], "mix_out",
    )
    grad_tokens, grad_wout, gpack, grad_win, ggains = finish_call(
        gpart, gwout, gw, gpack, tokens, grad_resid, gains, grad_gmoe[None], n_seq, 9
    )
    own = gain_mix.shape[0]
    ggains = lax.dynamic_slice(
        ggains, (0, (lax.axis_index("dp") * n_seq + lax.axis_index("seq")) * own), (2, own)
    )
    return (
        result, grad_tokens, ggains[0], grad_win, gpack[:, 256:260], gpack[:, :n_small],
        gpack[:, 128 : 128 + rank], gpack[:, 264], gpack[:, 272 : 272 + NS], gpack[:, 265],
        grad_wout, ggains[1], grad_up[None], grad_down[None],
    )


def solution(mesh):
    row2, row1 = P(("dp", "seq"), None), P(("dp", "seq"))
    mats = P("dp", "seq", None)
    return jax.shard_map(
        on_device,
        mesh=mesh,
        in_specs=(
            row2, row2, row2, row1, row2, row2, row2, row2, row1, row2, row1, row2, row1, mats, mats
        ),
        out_specs=(
            row2, row2, row1, row2, row2, row2, row2, row1, row2, row1, row2, row1, mats, mats
        ),
        check_vma=False,
    )
```

```python
from functools import partial

import jax
import jax.numpy as jnp
from jax import lax
from jax.experimental import pallas as pl
from jax.experimental.pallas import tpu as pltpu
from jax.sharding import PartitionSpec as P

NS = 16
B_AT, C_AT = 80, 96
LN2 = 0.6931471805599453
LOG2E = 1.4426950408889634
eps = 1e-05
f32 = jnp.float32
bf16 = jnp.bfloat16

NN = (((1,), (0,)), ((), ()))
NT = (((1,), (1,)), ((), ()))
TN = (((0,), (0,)), ((), ()))


def mm(left, right, dims=NN):
    return lax.dot_general(left, right, dims, preferred_element_type=f32)


def up128(count):
    return -(-count // 128) * 128


def rms_norm(values, gain_vec):
    return values * lax.rsqrt(jnp.mean(values * values, axis=-1, keepdims=True) + eps) * gain_vec


def sigmoid(v):
    return 1.0 / (1.0 + jnp.exp(-v))


def softplus(v):
    return jnp.maximum(v, 0.0) + jnp.log1p(jnp.exp(-jnp.abs(v)))


def tree_step(first, second, by):
    row = lax.broadcasted_iota(jnp.int32, first.shape, 0)
    clear = (row & by) == 0
    return jnp.where(clear, first, second) + pltpu.roll(jnp.where(clear, second, first), by, 0)


def tree_push(stack, value, falling=False):
    level = 1
    while stack and stack[-1][0] == level:
        other = stack.pop()[1]
        value = tree_step(value, other, level) if falling else tree_step(other, value, level)
        level *= 2
    stack.append((level, value))


def turned(misc):
    return misc[...].astype(f32).T


def in_kernel(
    n_seq, steps, tok, gain, w, wx, misc, cot_own, x_out, z_out, conv_out, norm_out, small_all, cot_all,
    buf, mt, csem, *scratch,
):
    rows, cp = x_out.shape
    line = Line(n_seq)
    sums = Sum(line, scratch[7:], small_all)
    half = cot_own.shape[0] // 2
    slots_of = Gather(
        line, lambda q, p: cot_all.at[q, p], lambda p: cot_own.at[p], range(half), scratch[:7]
    )
    own = pltpu.make_async_copy(cot_own, cot_all.at[line.me], csem)

    @pl.when(pl.program_id(0) == 0)
    def _():
        greet([(None, q) for q in all_peers(n_seq)])
        own.start()
        slots_of.stage(0)

    late = []
    for k in range(1, line.n):
        at = k * steps // (line.n - 1) + 1
        if at < steps:
            pl.when(pl.program_id(0) == at)(lambda k=k: slots_of.stage(k))
        else:
            late.append(k)

    @pl.when(pl.program_id(0) == 0)
    def _():
        buf[0:8, :] = jnp.zeros((8, cp), f32)
        mt[...] = turned(misc)

    @pl.when(pl.program_id(0) > 0)
    def _():
        buf[0:8, :] = buf[rows : rows + 8, :]

    normed = rms_norm(tok[...].astype(f32), gain[0:1, :]).astype(bf16)
    norm_out[...] = normed
    prod = mm(normed, w[...])
    x_part = prod[:, :cp]
    x_out[...] = x_part
    z_out[...] = prod[:, cp:]
    buf[8 : 8 + rows, :] = x_part
    conv = x_part * mt[3:4, :]
    for k in range(3):
        conv = conv + buf[5 + k : 5 + k + rows, :] * mt[k : k + 1, :]
    conv_out[...] = conv
    sums.put(pl.program_id(0), mm((conv * sigmoid(conv)).astype(bf16), wx[...]))

    @pl.when(pl.program_id(0) == steps - 1)
    def _():
        sums.finish()
        for k in late:
            slots_of.stage(k)
        slots_of.finish()
        own.wait()


def stage_step(k, n, steps):
    return steps - 1 - (n - 1 - k) * max(1, (steps - 2) // max(1, n - 1))


def state_maps(small, st):
    st[...] = small[...].astype(f32).T[B_AT : B_AT + 2 * NS, :]


def maps_of(st, g):
    lanes = st.shape[1]
    return pltpu.roll(st[...], lax.rem(lanes - 8 * g, lanes), 1)


def scan_kernel(
    n_seq, steps, small, wdt, misc, conv, z, wout, cot_own, cot_half,
    dtp_out, delta_out, u_out, h_out, ssm_out, gated_out, mixed, cot_all,
    du_s, state, mt, a2, st, *sems,
):
    rows, cp = conv.shape
    line = Line(n_seq)
    step = pl.program_id(0)
    slots_of = Gather(
        line, lambda q, p: cot_all.at[q, p], lambda p: cot_own.at[p],
        range(cot_own.shape[0] // 2, cot_own.shape[0]), sems[:7],
    )

    def final(p, value):
        high = value.shape[0]
        mixed[p * high : (p + 1) * high, :] = value

    stream = Made(line, sems[7:], final)

    @pl.when(step == 0)
    def _():
        greet(line.neighbours())
        slots_of.stage(0)
        state[...] = jnp.zeros_like(state)
        mt[...] = turned(misc)
        a2[...] = -jnp.exp(mt[16:32, :]) * LOG2E

    for k in range(1, line.n):
        pl.when(step == k * steps // line.n)(lambda k=k: slots_of.stage(k))

    dtp = mm(small[...], wdt[...], NT) + mt[8:9, :]
    dtp_out[...] = dtp
    delta = softplus(dtp)
    cv = conv[...]
    u = cv * sigmoid(cv)
    u_out[...] = u
    delta_out[...] = delta
    du_s[...] = delta * u
    state_maps(small, st)

    def group(g, h):
        base = pl.multiple_of(g * 8, 8)
        bc = maps_of(st, g)
        stack = []
        for t in range(8):
            d = jnp.broadcast_to(delta_out[pl.ds(base + t, 1), :], (NS, cp))
            du = jnp.broadcast_to(du_s[pl.ds(base + t, 1), :], (NS, cp))
            h = jnp.exp2(d * a2[...]) * h + du * bc[:NS, t : t + 1]
            h_out[base + t] = h
            prod = h * bc[NS:, t : t + 1]
            tree_push(stack, prod[:8] + prod[8:])
        ssm_out[pl.ds(base, 8), :] = stack[0][1]
        return h

    state[...] = lax.fori_loop(0, rows // 8, group, state[...], unroll=2)
    zv = z[...]
    gated = (ssm_out[...] + mt[9:10, :] * u) * (zv * sigmoid(zv))
    low = gated.astype(bf16)
    gated_out[...] = low
    stream.put(step, mm(low, wout[...]))

    @pl.when(step == steps - 1)
    def _():
        for t in range(line.n):
            stream.stage(t)
        stream.finish()
        slots_of.finish()


def cut_rows(src, out):
    parts, blocks, high, _ = out.shape
    for b in range(parts * blocks):
        out[b // blocks, b % blocks] = src[b * high : (b + 1) * high, :].astype(out.dtype)


def back_kernel(
    n_seq, steps, gml, wout, gated, u_ref, z, ssm, delta_ref, dtp, hs, hlast, small, wdt, misc, term,
    norm, gu_out, gz_out, gwout_out, gwdt, gmisc, gwz_out, sums_out, small_all,
    du_s, gs_s, r1_s, r2_s, lam_s, mt, a2, st, lams, gwout, ga, gwz, *scratch,
):
    rows, cp = u_ref.shape
    step = pl.program_id(0)
    last = steps - 1
    line = Line(n_seq)
    work = Collect(line, term, sums_out, scratch[:-8])
    sums = Sum(line, scratch[-8:], small_all)

    @pl.when(step == 0)
    def _():
        greet([(None, q) for q in all_peers(n_seq)], work.peers)
        work.open()
        lam_s[...] = jnp.zeros_like(lam_s)
        gwout[...] = jnp.zeros_like(gwout)
        gwz[...] = jnp.zeros_like(gwz)
        gwdt[...] = jnp.zeros_like(gwdt)
        ga[...] = jnp.zeros_like(ga)
        gmisc[...] = jnp.zeros_like(gmisc)
        mt[...] = turned(misc)
        a2[...] = -jnp.exp(mt[16:32, :]) * LOG2E

    for t in range(line.n):
        at = 2 + t * (steps - 4) // max(1, line.n - 1)
        pl.when(step == at)(lambda t=t: work.stage(t))

    grad_mixed = gml[...]
    gg = mm(grad_mixed, wout[...], NT)
    gwout[...] += mm(gated[...], grad_mixed, TN)
    zv = z[...]
    sz = sigmoid(zv)
    u = u_ref[...]
    skip = mt[9:10, :]
    gz = (gg * (ssm[...] + skip * u) * (sz * (1.0 + zv * (1.0 - sz)))).astype(bf16)
    gz_out[...] = gz
    gwz[...] += mm(norm[...], gz, TN)
    gs = gg * (zv * sz)
    gs_s[...] = gs
    du_s[...] = delta_ref[...] * u
    state_maps(small, st)
    keep_first = jnp.where(step == last, 0.0, 1.0)

    def group(k, carry):
        lamd, acc = carry
        g = rows // 8 - 1 - k
        base = pl.multiple_of(g * 8, 8)
        bc = maps_of(st, g)
        stack1, stack2 = [], []
        for t in range(7, -1, -1):
            d = jnp.broadcast_to(delta_ref[pl.ds(base + t, 1), :], (NS, cp))
            g_s = jnp.broadcast_to(gs_s[pl.ds(base + t, 1), :], (NS, cp))
            if t > 0:
                before = hs[base + t - 1]
            else:
                inside = hs[jnp.maximum(base - 1, 0)]
                before = jnp.where(g == 0, hlast[0] * keep_first, inside)
            lam = lamd + g_s * bc[NS:, t : t + 1]
            lams[base + t] = lam.astype(bf16)
            lamd = jnp.exp2(d * a2[...]) * lam
            w = lamd * before
            acc = acc + w * d
            wa = w * a2[...]
            lb = lam * bc[:NS, t : t + 1]
            tree_push(stack1, wa[:8] + wa[8:], True)
            tree_push(stack2, lb[:8] + lb[8:], True)
        r1_s[pl.ds(base, 8), :] = stack1[0][1]
        r2_s[pl.ds(base, 8), :] = stack2[0][1]
        return lamd, acc

    lamd, acc = lax.fori_loop(0, rows // 8, group, (lam_s[...], jnp.zeros((NS, cp), f32)), unroll=2)
    lam_s[...] = lamd
    ga[...] += acc
    r2 = r2_s[...]
    gu_out[...] = skip * gs + delta_ref[...] * r2
    gdelta = r1_s[...] * LN2 + u * r2
    gdtp = gdelta * sigmoid(dtp[...])
    gmisc[8:9, :] += jnp.sum(gdtp, axis=0, keepdims=True)
    gmisc[9:10, :] += jnp.sum(gs * u, axis=0, keepdims=True)
    low = gdtp.astype(bf16)
    gwdt[...] += mm(low, small[...], TN)

    lane = lax.broadcasted_iota(jnp.int32, (8, 128), 1)
    same = lax.broadcasted_iota(jnp.int32, (8, 128), 0) == lane // NS

    def of_channels(values, states):
        prod = jnp.where(same, mm(values.astype(bf16), states, NT), 0.0)
        for by in (64, 32, 16):
            prod = prod + pltpu.roll(prod, by, 1)
        return prod

    parts = []
    for g in range(rows // 8):
        own8 = slice(g * 8, g * 8 + 8)
        gb = of_channels(du_s[own8, :], lams[own8].reshape(8 * NS, cp))
        gc = of_channels(gs_s[own8, :], hs[own8].reshape(8 * NS, cp).astype(bf16))
        parts.append(jnp.where(lane < C_AT, gb, gc))
    grad_bc = jnp.concatenate(parts, axis=0)
    wide = lax.broadcasted_iota(jnp.int32, (rows, 128), 1)
    grad_bc = jnp.where(jnp.logical_and(wide >= B_AT, wide < C_AT + NS), grad_bc, 0.0)
    sums.put(steps - 1 - step, mm(low, wdt[...]) + grad_bc)

    @pl.when(step == last)
    def _():
        gmisc[16:32, :] = ga[...] * (a2[...] * LN2)
        parts, cpd, _ = gwout_out.shape
        for p in range(parts):
            gwout_out[p] = gwout[p * cpd : (p + 1) * cpd, :].astype(bf16)
        cut_rows(gwz, gwz_out)
        sums.finish()
        work.finish()


def out_kernel(
    n_seq, steps, gsmall, wx, misc, conv, x, gu, gz, norm, w, gwdt, gmisc, gwout, gwz, tok, gres, gains, ggmoe,
    gtok_out, gwout_out, pack_sum, gwin_out, gain_out,
    buf, mt, gwx, gw, gm, gw_out, pack_out, *scratch,
):
    rows, cp = conv.shape
    step = pl.program_id(0)
    final = Finish(
        n_seq, gwout, gwz, gw_out, pack_out, tok, gres, gains, ggmoe,
        gtok_out, gwout_out, pack_sum, gwin_out, gain_out, *scratch,
    )
    pl.when(step == 0)(final.open)
    pl.when(step == 2)(final.early_middle)
    pl.when(step == steps - 2)(final.early_final)

    @pl.when(pl.program_id(0) == 0)
    def _():
        buf[rows : rows + 8, :] = jnp.zeros((8, cp), f32)
        gwx[...] = jnp.zeros_like(gwx)
        gw[...] = jnp.zeros_like(gw)
        gm[...] = jnp.zeros_like(gm)
        gm[8:32, :] = gmisc[8:32, :]
        mt[...] = turned(misc)

    @pl.when(pl.program_id(0) > 0)
    def _():
        buf[rows : rows + 8, :] = buf[0:8, :]

    gsl = gsmall[...]
    cv = conv[...]
    s = sigmoid(cv)
    gwx[...] += mm((cv * s).astype(bf16), gsl, TN)
    gconv = (gu[...] + mm(gsl, wx[...], NT)) * (s * (1.0 + cv * (1.0 - s)))
    buf[0:rows, :] = gconv
    xv = x[...]
    gx = gconv * mt[3:4, :]
    gm[3:4, :] += jnp.sum(gconv * xv, axis=0, keepdims=True)
    for k in range(3):
        moved = buf[3 - k : 3 - k + rows, :]
        gx = gx + moved * mt[k : k + 1, :]
        gm[k : k + 1, :] += jnp.sum(moved * xv, axis=0, keepdims=True)
    gx = gx.astype(bf16)
    gp = jnp.concatenate([gx, gz[...]], axis=1)
    final.stream.put(steps - 1 - step, mm(gp, w[...], NT))
    gw[...] += mm(norm[...], gx, TN)

    @pl.when(pl.program_id(0) == pl.num_programs(0) - 1)
    def _():
        cut_rows(gw, gw_out)
        final.f_w.start()
        flat = gm[...].T
        parts, cpd, _ = pack_out.shape
        for p in range(parts):
            own = slice(p * cpd, (p + 1) * cpd)
            pack_out[p, :, 0:128] = gwx[own, :]
            pack_out[p, :, 128:256] = gwdt[own, :]
            pack_out[p, :, 256:384] = flat[own, :]
        final.close()


def chunked(kernel, steps, backward, ins, outs, scratch, name, number=None, alias=None):
    def at(i):
        return steps - 1 - i if backward else i

    def spec(shape, rows):
        tail = (0,) * (len(shape) - 1)
        if rows is None:
            return pl.BlockSpec(memory_space=pl.ANY)
        if isinstance(rows, tuple):
            (block, column), = rows
            return pl.BlockSpec(block, lambda i: (0, column))
        if rows == 0:
            return pl.BlockSpec(shape, lambda i: (0,) + tail)
        if rows < 0:
            return pl.BlockSpec((1,) + shape[1:], lambda i: (jnp.maximum(at(i) * -rows - 1, 0),) + tail)
        return pl.BlockSpec((rows,) + shape[1:], lambda i: (at(i),) + tail)

    return pl.pallas_call(
        kernel,
        grid=(steps,),
        in_specs=[spec(a.shape, r) for a, r in ins],
        out_specs=[spec(s.shape, r) for s, r in outs],
        out_shape=[s for s, _ in outs],
        scratch_shapes=scratch,
        name=name,
        input_output_aliases=alias or {},
        compiler_params=pltpu.CompilerParams(
            dimension_semantics=("arbitrary",), vmem_limit_bytes=60 * 1024 * 1024,
            collective_id=number, has_side_effects=number is not None,
        ),
    )(*[a for a, _ in ins])


MESH = pl.DeviceIdType.MESH


def remote(src, dst, send, recv, **where):
    return pltpu.make_async_remote_copy(
        src_ref=src, dst_ref=dst, send_sem=send, recv_sem=recv, device_id=where, device_id_type=MESH
    )


class Line:
    def __init__(self, n_seq):
        assert n_seq % 2 == 0
        self.n = n_seq // 2
        self.n_seq = n_seq
        self.me = lax.axis_index("seq")
        self.o, self.i = self.me // 2, self.me % 2

    def at(self, o, i):
        return o * 2 + i

    def neighbours(self):
        return [
            (None, self.at(self.o, 1 - self.i)),
            (self.o > 0, self.at(self.o - 1, self.i)),
            (self.o < self.n - 1, self.at(self.o + 1, self.i)),
        ]

    def order(self, t):
        table = [
            sorted(range(self.n), key=lambda q, o=o: (-abs(q - o), -q))[t] for o in range(self.n)
        ]
        place = jnp.int32(0)
        for o in range(self.n):
            place = place + jnp.where(self.o == o, table[o], 0)
        return place


def when(condition, action):
    if condition is None:
        action()
    else:
        pl.when(condition)(action)


def greet(peers, extra=()):
    barrier = pltpu.get_barrier_semaphore()
    count = jnp.int32(0)
    for condition, place in peers:
        when(
            condition,
            lambda place=place: pl.semaphore_signal(
                barrier, inc=1, device_id={"seq": place}, device_id_type=MESH
            ),
        )
        count = count + (1 if condition is None else jnp.where(condition, 1, 0))
    for place in extra:
        pl.semaphore_signal(barrier, inc=1, device_id={"dp": place}, device_id_type=MESH)
        count = count + 1
    pl.semaphore_wait(barrier, count)


def gather_sems(n, pieces):
    dma = pltpu.SemaphoreType.DMA
    return [
        dma((n, pieces)), dma((pieces,)), dma((n, pieces)), dma((n, pieces)), dma((n, pieces)),
        dma((2, pieces)), dma((pieces,)),
    ]


class Gather:
    def __init__(self, line, at, own, pieces, sems):
        self.line, self.at, self.own, self.pieces, self.sems = line, at, own, pieces, sems

    def copy(self, src, q, p, send, recv, place):
        return remote(src, self.at(self.line.at(q, self.line.i), p), send, recv, seq=place)

    def up(self, src, q, p):
        zs, _, zr = self.sems[:3]
        return self.copy(src, q, p, zs.at[q, p], zr.at[q, p], self.line.at(self.line.o + 1, self.line.i))

    def down(self, src, q, p, own):
        zs, zd, zr = self.sems[:3]
        send = zd.at[p] if own else zs.at[q, p]
        return self.copy(src, q, p, send, zr.at[q, p], self.line.at(self.line.o - 1, self.line.i))

    def over(self, src, q, p):
        ys, yr = self.sems[3:5]
        return self.copy(src, q, p, ys.at[q, p], yr.at[q, p], self.line.at(self.line.o, 1 - self.line.i))

    def late(self, p):
        pieces = list(self.pieces)
        return self.line.n > 2 and pieces.index(p) >= (len(pieces) + 1) // 2

    def extra(self, end, p):
        line = self.line
        far, to = (line.n - 1, 0) if end == 0 else (0, line.n - 1)
        here = self.at(line.at(far, 1 - line.i), p)
        return remote(here, here, self.sems[5].at[end, p], self.sems[6].at[p], seq=line.at(to, line.i))

    def each(self, k, act, arrive=None):
        line, o, n = self.line, self.line.o, self.line.n
        for p in self.pieces:
            if k == 0:
                src = self.own(p)
                if arrive is not None:
                    arrive(p)
                pl.when(o < n - 1)(lambda src=src, p=p: act(self.up(src, o, p)))
                pl.when(o > 0)(lambda src=src, p=p: act(self.down(src, o, p, True)))
                act(self.over(src, o, p))
                continue

            def below(p=p):
                q = o - k
                src = self.at(line.at(q, line.i), p)
                if arrive is not None:
                    arrive(self.up(src, q, p))
                if k < n - 1:
                    pl.when(o < n - 1)(lambda: act(self.up(src, q, p)))
                if k < n - 1 or not self.late(p):
                    act(self.over(src, q, p))

            def above(p=p):
                q = o + k
                src = self.at(line.at(q, line.i), p)
                if arrive is not None:
                    arrive(self.up(src, q, p))
                if k < n - 1:
                    pl.when(o > 0)(lambda: act(self.down(src, q, p, False)))
                if k < n - 1 or not self.late(p):
                    act(self.over(src, q, p))

            if arrive is not None or k < n - 1 or not self.late(p):
                pl.when(o >= k)(below)
                pl.when(o + k <= n - 1)(above)

    def stage(self, k, ready=None):
        arrive = ready if k == 0 else (lambda copy: copy.wait_recv())
        self.each(k, lambda copy: copy.start(), arrive)

    def finish(self):
        line = self.line
        o, n = line.o, line.n
        ends = ((0, n - 1, 1, 0), (1, 0, n - 2, n - 1))
        held = [p for p in self.pieces if self.late(p)]

        def over_in(q, p):
            self.over(self.at(line.at(q, 1 - line.i), p), q, p).wait_recv()

        for end, far, beside, _ in ends:
            for p in held:
                @pl.when(o == beside)
                def _(end=end, far=far, p=p):
                    over_in(far, p)
                    self.extra(end, p).start()

        for q in range(n):
            for p in self.pieces:
                if p in held and q in (0, n - 1):
                    end, _, beside, at = ends[0 if q == n - 1 else 1]
                    done = jnp.logical_or(o == beside, o == at)
                    pl.when(jnp.logical_not(done))(lambda q=q, p=p: over_in(q, p))
                    pl.when(o == at)(lambda end=end, p=p: self.extra(end, p).wait_recv())
                else:
                    over_in(q, p)
        for end, _, beside, _ in ends:
            for p in held:
                pl.when(o == beside)(lambda end=end, p=p: self.extra(end, p).wait_send())
        for k in range(n):
            self.each(k, lambda copy: copy.wait_send())

    def run(self, ready=None):
        for k in range(self.line.n):
            self.stage(k, ready)
        self.finish()


def gather_kernel(n_seq, x, out, lsem, *sems):
    line = Line(n_seq)
    greet(line.neighbours())
    keep = pltpu.make_async_copy(x, out.at[line.me], lsem)
    keep.start()
    Gather(line, lambda q, p: out.at[q, p], lambda p: x.at[p], range(x.shape[0]), sems).run()
    keep.wait()


def seq_gather(x, n_seq, pieces, number):
    rows, width = x.shape
    out = pl.pallas_call(
        partial(gather_kernel, n_seq),
        in_specs=[pl.BlockSpec(memory_space=pl.ANY)],
        out_specs=pl.BlockSpec(memory_space=pl.ANY),
        out_shape=jax.ShapeDtypeStruct((n_seq, pieces, rows // pieces, width), x.dtype),
        scratch_shapes=[pltpu.SemaphoreType.DMA] + gather_sems(n_seq // 2, pieces),
        compiler_params=pltpu.CompilerParams(collective_id=number, has_side_effects=True),
        name="seq_gather",
    )(x.reshape(pieces, rows // pieces, width))
    return out.reshape(n_seq * rows, width)


def dispatch_kernel(n_seq, n_dp, x, out, lsem, dps, dpr, *sems):
    line = Line(n_seq)
    mine = lax.axis_index("dp")
    peers = [lax.rem(mine + r, n_dp) for r in range(1, n_dp)]
    greet(line.neighbours(), peers)
    copies = []
    for r, peer in enumerate(peers):
        copy = remote(x.at[peer], out.at[line.me, mine], dps.at[r], dpr.at[r], dp=peer)
        copy.start()
        copies.append(copy)
    keep = pltpu.make_async_copy(x.at[mine], out.at[line.me, mine], lsem)
    keep.start()

    def ready(r):
        if r == 0:
            keep.wait()
        else:
            source = out.at[line.me, lax.rem(mine + n_dp - r, n_dp)]
            remote(source, source, dps.at[r - 1], dpr.at[r - 1], dp=peers[r - 1]).wait_recv()

    at = rolled(out, mine, n_dp)
    Gather(line, at, lambda r: at(line.me, r), range(n_dp), sems).run(ready)
    for copy in copies:
        copy.wait_send()


def rolled(out, mine, n_dp):
    return lambda q, r: out.at[q, lax.rem(mine + n_dp - r, n_dp)]


def dispatch_call(x, n_seq, number):
    n_dp, rows, width = x.shape
    dma = pltpu.SemaphoreType.DMA
    return pl.pallas_call(
        partial(dispatch_kernel, n_seq, n_dp),
        in_specs=[pl.BlockSpec(memory_space=pl.ANY)],
        out_specs=pl.BlockSpec(memory_space=pl.ANY),
        out_shape=jax.ShapeDtypeStruct((n_seq, n_dp, rows, width), x.dtype),
        scratch_shapes=[dma, dma((n_dp - 1,)), dma((n_dp - 1,))] + gather_sems(n_seq // 2, n_dp),
        compiler_params=pltpu.CompilerParams(collective_id=number, has_side_effects=True),
        name="dispatch",
    )(x)


def scatter_scratch(n, pieces, rows, width):
    dma = pltpu.SemaphoreType.DMA
    return [
        pltpu.VMEM((n, pieces, rows, width), bf16),
        pltpu.VMEM((n, pieces, rows, width), bf16),
        pltpu.VMEM((n + 1, pieces, rows, width), bf16),
        dma((n, pieces)), dma((n, pieces)), dma((n, pieces)), dma((n + 1, pieces)),
    ]


class Scatter:
    def __init__(self, line, at, pieces, scratch, final):
        self.line, self.at, self.pieces, self.final = line, at, pieces, final
        self.ybuf, self.zout, self.zin, self.ys, self.yr, self.zs, self.zr = scratch

    def over(self, t, p):
        q, line = self.line.order(t), self.line
        return remote(self.at(line.at(q, 1 - line.i), p), self.ybuf.at[q, p], self.ys.at[q, p],
                      self.yr.at[q, p], seq=line.at(line.o, 1 - line.i))

    def along(self, t, p):
        q, line = self.line.order(t), self.line
        up = q > line.o
        to = jnp.where(up, line.o + 1, line.o - 1)
        slot = jnp.where(jnp.logical_and(q == to, jnp.logical_not(up)), line.n, q)
        return remote(self.zout.at[q, p], self.zin.at[slot, p], self.zs.at[q, p], self.zr.at[slot, p],
                      seq=line.at(to, line.i))

    def arrived(self, k, p):
        here, line = self.zin.at[k, p], self.line
        remote(here, here, self.zs.at[0, p], self.zr.at[k, p],
               seq=line.at(line.o, 1 - line.i)).wait_recv()

    def open(self):
        for t in range(self.line.n):
            for p in self.pieces:
                self.over(t, p).start()

    def stage(self, t):
        line = self.line
        o, n = line.o, line.n
        q = line.order(t)
        for p in self.pieces:
            self.over(t, p).wait_recv()
            value = self.at(line.at(q, line.i), p)[...].astype(f32) + self.ybuf[q, p].astype(f32)
            if t < n - 1:
                fed = jnp.where(q > o, o > 0, o < n - 1)

                def with_feed(value=value, p=p):
                    self.arrived(q, p)
                    self.zout[q, p] = (value + self.zin[q, p].astype(f32)).astype(bf16)

                def without(value=value, p=p):
                    self.zout[q, p] = value.astype(bf16)

                pl.when(fed)(with_feed)
                pl.when(jnp.logical_not(fed))(without)
                self.along(t, p).start()
            else:
                below, above = o > 0, o < n - 1
                pl.when(below)(lambda p=p: self.arrived(o, p))
                pl.when(above)(lambda p=p: self.arrived(n, p))
                value = value + jnp.where(below, self.zin[o, p].astype(f32), 0.0)
                value = value + jnp.where(above, self.zin[n, p].astype(f32), 0.0)
                self.final(p, value)

    def finish(self):
        for t in range(self.line.n):
            for p in self.pieces:
                self.over(t, p).wait_send()
                if t < self.line.n - 1:
                    self.along(t, p).wait_send()

    def run(self):
        self.open()
        for t in range(self.line.n):
            self.stage(t)
        self.finish()


def scatter_kernel(n_seq, term, out, *scratch):
    line = Line(n_seq)
    greet(line.neighbours())

    def final(p, value):
        out[p] = value

    Scatter(line, lambda q, p: term.at[q, p], range(term.shape[1]), scratch, final).run()


def seq_scatter(x, n_seq, pieces, number):
    rows, width = x.shape[0] // n_seq, x.shape[1]
    part = rows // pieces
    vmem = pl.BlockSpec(memory_space=pltpu.VMEM)
    out = pl.pallas_call(
        partial(scatter_kernel, n_seq),
        in_specs=[vmem],
        out_specs=vmem,
        out_shape=jax.ShapeDtypeStruct((pieces, part, width), f32),
        scratch_shapes=scatter_scratch(n_seq // 2, pieces, part, width),
        compiler_params=pltpu.CompilerParams(
            collective_id=number, has_side_effects=True, vmem_limit_bytes=60 * 1024 * 1024
        ),
        name="seq_scatter",
    )(x.reshape(n_seq, pieces, part, width))
    return out.reshape(rows, width)


class Collect:
    def __init__(self, line, term, out, scratch):
        self.line, self.term, self.out = line, term, out
        self.sumbuf, self.lsem, self.dps, self.dpr = scratch[:4]
        self.n_dp = term.shape[1]
        self.mine = lax.axis_index("dp")
        self.peers = [lax.rem(self.mine + r, self.n_dp) for r in range(1, self.n_dp)]

        def at(q, r):
            return term.at[q, lax.rem(self.mine + r, self.n_dp)]

        def final(r, value):
            self.sumbuf[r] = value.astype(bf16)
            self.back(r).start()

        pieces = list(range(1, self.n_dp)) + [0]
        self.scatter = Scatter(line, at, pieces, scratch[4:], final)
        self.open, self.stage = self.scatter.open, self.scatter.stage

    def back(self, r):
        if r == 0:
            return pltpu.make_async_copy(self.sumbuf.at[0], self.out.at[self.mine], self.lsem)
        return remote(self.sumbuf.at[r], self.out.at[self.mine], self.dps.at[r - 1], self.dpr.at[r - 1],
                      dp=self.peers[r - 1])

    def finish(self):
        self.scatter.finish()
        for r in range(1, self.n_dp):
            here = self.out.at[lax.rem(self.mine + self.n_dp - r, self.n_dp)]
            remote(here, here, self.dps.at[r - 1], self.dpr.at[r - 1],
                   dp=self.peers[r - 1]).wait_recv()
            self.back(r).wait_send()
        self.back(0).wait()


def collect_scratch(n_seq, n_dp, rows, width):
    dma = pltpu.SemaphoreType.DMA
    return [pltpu.VMEM((n_dp, rows, width), bf16), dma, dma((n_dp - 1,)), dma((n_dp - 1,))] + (
        scatter_scratch(n_seq // 2, n_dp, rows, width)
    )


def collect_kernel(n_seq, term, out, *scratch):
    line = Line(n_seq)
    work = Collect(line, term, out, scratch)
    greet(line.neighbours(), work.peers)
    work.open()
    for t in range(line.n):
        work.stage(t)
    work.finish()


def collect_call(x, n_seq, number):
    _, n_dp, rows, width = x.shape
    vmem = pl.BlockSpec(memory_space=pltpu.VMEM)
    return pl.pallas_call(
        partial(collect_kernel, n_seq),
        in_specs=[vmem],
        out_specs=vmem,
        out_shape=jax.ShapeDtypeStruct((n_dp, rows, width), bf16),
        scratch_shapes=collect_scratch(n_seq, n_dp, rows, width),
        compiler_params=pltpu.CompilerParams(
            collective_id=number, has_side_effects=True, vmem_limit_bytes=60 * 1024 * 1024
        ),
        name="collect",
    )(x)


def made_scratch(n, pieces, rows, width):
    return [pltpu.VMEM((2 * n, pieces, rows, width), bf16)] + scatter_scratch(n, pieces, rows, width)


class Made(Scatter):
    def __init__(self, line, scratch, final):
        self.made = scratch[0]
        pieces = self.made.shape[1]
        super().__init__(line, lambda q, p: self.made.at[q, p], range(pieces), scratch[1:], final)

    def put(self, b, value):
        line, rows = self.line, self.made.shape[2]
        for p in self.pieces:
            self.made[b, p] = value[p * rows : (p + 1) * rows, :].astype(bf16)

        @pl.when(b % 2 != line.i)
        def _():
            for p in self.pieces:
                remote(self.made.at[b, p], self.ybuf.at[b // 2, p], self.ys.at[b // 2, p],
                       self.yr.at[b // 2, p], seq=line.at(line.o, 1 - line.i)).start()


def sum_scratch(n_seq, rows, width):
    dma = pltpu.SemaphoreType.DMA
    mem = pltpu.VMEM
    return [
        mem((n_seq, rows, width), bf16), mem((n_seq, rows, width), bf16), mem((rows, width), bf16),
        dma, dma((n_seq,)), dma((n_seq,)), dma((n_seq,)), dma((n_seq,)),
    ]


class Sum:
    def __init__(self, line, scratch, out):
        self.line, self.out = line, out
        self.made, self.inbox, self.total, self.own, self.s1, self.r1, self.s2, self.r2 = scratch

    def send(self, b):
        me = self.line.me
        return remote(self.made.at[b], self.inbox.at[me], self.s1.at[b], self.r1.at[me], seq=b)

    def spread(self, q):
        me = self.line.me
        return remote(self.total, self.out.at[me], self.s2.at[q], self.r2.at[me], seq=q)

    def put(self, b, value):
        self.made[b] = value.astype(bf16)
        pl.when(b != self.line.me)(lambda: self.send(b).start())

    def finish(self):
        me = self.line.me
        peers = all_peers(self.line.n_seq)
        value = self.made[me].astype(f32)
        for q in peers:
            here = self.inbox.at[q]
            remote(here, here, self.s1.at[q], self.r1.at[q], seq=q).wait_recv()
            value = value + self.inbox[q].astype(f32)
        self.total[...] = value.astype(bf16)
        for q in peers:
            self.spread(q).start()
        own = pltpu.make_async_copy(self.total, self.out.at[me], self.own)
        own.start()
        for q in peers:
            here = self.out.at[q]
            remote(here, here, self.s2.at[q], self.r2.at[q], seq=q).wait_recv()
        own.wait()
        for q in peers:
            self.send(q).wait_send()
            self.spread(q).wait_send()


def all_peers(n_seq):
    me = lax.axis_index("seq")
    return [lax.rem(me + r, n_seq) for r in range(1, n_seq)]


def dp_peers():
    mine = lax.axis_index("dp")
    other = mine + 1 - 2 * lax.rem(mine, 2)
    return mine, other, lax.rem(mine + 2, 4), lax.rem(other + 2, 4)


class Spread:
    def __init__(self, out, sems):
        self.out, (self.s, self.r) = out, sems
        self.mine, self.core, self.far, self.rest = dp_peers()
        self.sent = []

    def push(self, src, place, k, peer):
        copy = remote(src, self.out.at[place], self.s.at[k], self.r.at[k], dp=peer)
        copy.start()
        self.sent.append(copy)

    def wait(self, place, k):
        here = self.out.at[place]
        remote(here, here, self.s.at[k], self.r.at[k], dp=self.core).wait_recv()

    def start(self, src):
        self.push(src, self.mine, 1, self.far)
        self.push(src, self.mine, 0, self.core)

    def forward(self):
        self.wait(self.far, 1)
        self.push(self.out.at[self.far], self.far, 2, self.core)

    def finish(self):
        self.wait(self.core, 0)
        self.wait(self.rest, 2)
        for copy in self.sent:
            copy.wait_send()


def start_kernel(
    n_seq, tok, w_in, wout, side, gains, route, cot,
    xg, w_all, wout_all, side_all, gain_all, cot_own, pick_out,
    wst, gbox, zero_w, zero_s, cst, lsem, tsem, csem, cds, cdr, *sems,
):
    gsems, (a2s, a2r, gs2, gr2), dsems = sems[:7], sems[7:11], sems[11:]
    line = Line(n_seq)
    me = line.me
    peers = all_peers(n_seq)
    mine, core, far, rest = dp_peers()
    greet([(None, q) for q in peers], [core, far, rest])
    keep = pltpu.make_async_copy(tok, xg.at[me], tsem)
    keep.start()
    tokens_of = Gather(line, lambda q, p: xg.at[q, p], lambda p: tok.at[p], range(tok.shape[0]), gsems)
    tokens_of.stage(0)
    locals_ = []

    def local(src, dst, k):
        copy = pltpu.make_async_copy(src, dst, lsem.at[k])
        copy.start()
        locals_.append(copy)

    gain_dp = Spread(gbox, dsems[0:2])
    gbox[mine] = gains[...]
    gain_dp.start(gains)
    w_dp = Spread(w_all, dsems[2:4])
    wout_dp = Spread(wout_all, dsems[4:6])
    side_dp = Spread(side_all, dsems[6:8])
    side_dp.start(side)
    wout_dp.start(wout)
    local(wout, wout_all.at[mine], 0)
    local(side, side_all.at[mine], 1)
    zero_w[...] = jnp.zeros_like(zero_w)
    zero_s[...] = jnp.zeros_like(zero_s)

    here = route.shape[0]
    n_dp, slots, _ = cot_own.shape
    expert = lax.broadcasted_iota(jnp.int32, (here, n_dp), 1)
    onehot = jnp.where(route[...] == expert, 1.0, 0.0)
    earlier = lax.broadcasted_iota(jnp.int32, (here, here), 1) < lax.broadcasted_iota(
        jnp.int32, (here, here), 0
    )
    before = mm(jnp.where(earlier, 1.0, 0.0).astype(bf16), onehot.astype(bf16))
    index = jnp.sum(before * onehot, axis=1, keepdims=True)
    target = route[...] * slots + index.astype(jnp.int32)
    slot = lax.broadcasted_iota(jnp.int32, (here, n_dp * slots), 1)
    pick = jnp.where(target == slot, 1.0, 0.0).astype(bf16)
    pick_out[...] = pick
    for e in range(n_dp):
        cst[e] = mm(pick[:, e * slots : (e + 1) * slots], cot[...], TN).astype(bf16)
    copies = []
    for k, peer in enumerate((core, far, rest)):
        copy = remote(cst.at[peer], cot_own.at[mine], cds.at[k], cdr.at[k], dp=peer)
        copy.start()
        copies.append(copy)
    keep_cot = pltpu.make_async_copy(cst.at[mine], cot_own.at[mine], csem)
    keep_cot.start()

    high, wide = w_in.shape
    cpd = wide // (2 * 4 * n_seq)
    half = wst.shape[2] // 2
    values = w_in[...].astype(f32)
    for q in range(n_seq):
        for side_of in range(2):
            first = side_of * 4 * n_seq
            parts = [
                values[:, (first + p * n_seq + q) * cpd : (first + p * n_seq + q + 1) * cpd]
                for p in range(4)
            ]
            if half > 4 * cpd:
                parts.append(jnp.zeros((high, half - 4 * cpd), f32))
            wst[q, :, side_of * half : (side_of + 1) * half] = jnp.concatenate(
                parts, axis=1
            ).astype(bf16)
    for r, q in enumerate(peers):
        copy = remote(wst.at[q], w_all.at[mine, me], a2s.at[r], a2r.at[r], seq=q)
        copy.start()
        copies.append(copy)
    local(wst.at[me], w_all.at[mine, me], 2)
    extra = wout_all.shape[0] - 4
    for k in range(extra):
        local(zero_w, wout_all.at[4 + k], 3 + 2 * k)
        local(zero_s, side_all.at[4 + k], 4 + 2 * k)
    gain_dp.forward()
    gain_dp.finish()
    for r, q in enumerate(peers):
        copy = remote(gbox, gain_all.at[me], gs2.at[r], gr2.at[r], seq=q)
        copy.start()
        copies.append(copy)
    gain_all[me] = gbox[...]
    tokens_of.stage(1)
    for r, q in enumerate(peers):
        here = w_all.at[mine, lax.rem(me + n_seq - 1 - r, n_seq)]
        remote(here, here, a2s.at[r], a2r.at[r], seq=q).wait_recv()
    for copy in locals_:
        copy.wait()
    w_dp.start(w_all.at[mine])
    if line.n > 2:
        tokens_of.stage(2)
    side_dp.forward()
    wout_dp.forward()
    for k in range(3, line.n):
        tokens_of.stage(k)
    w_dp.forward()
    tokens_of.finish()
    side_dp.finish()
    wout_dp.finish()
    for r, q in enumerate(peers):
        here = gain_all.at[lax.rem(me + n_seq - 1 - r, n_seq)]
        remote(here, here, gs2.at[r], gr2.at[r], seq=q).wait_recv()
    for k, peer in enumerate((core, far, rest)):
        remote(cot_own.at[peer], cot_own.at[peer], cds.at[k], cdr.at[k], dp=peer).wait_recv()
    keep_cot.wait()
    keep.wait()
    w_dp.finish()
    for copy in copies:
        copy.wait_send()


def start_call(tokens, w_in, w_out, side, gains, route, cot, slots, n_seq, cp, number):
    here, d_model = tokens.shape
    high, _ = w_in.shape
    cpd, n_side = side.shape
    extra = -(-cp // cpd) - 4
    dma = pltpu.SemaphoreType.DMA
    anyw, vmem = pl.BlockSpec(memory_space=pl.ANY), pl.BlockSpec(memory_space=pltpu.VMEM)
    sds = jax.ShapeDtypeStruct
    return pl.pallas_call(
        partial(start_kernel, n_seq),
        in_specs=[anyw, vmem, anyw, anyw, vmem, vmem, vmem],
        out_specs=[anyw, anyw, anyw, anyw, vmem, anyw, vmem],
        out_shape=[
            sds((n_seq, 2, here // 2, d_model), bf16),
            sds((4, n_seq, high, 2 * cp), bf16),
            sds((4 + extra, cpd, d_model), bf16),
            sds((4 + extra, cpd, n_side), bf16),
            sds((n_seq, 4, 8, 128), f32),
            sds((4, slots, d_model), bf16),
            sds((here, 4 * slots), bf16),
        ],
        scratch_shapes=[
            pltpu.VMEM((n_seq, high, 2 * cp), bf16), pltpu.VMEM((4, 8, 128), f32),
            pltpu.VMEM((cpd, d_model), bf16), pltpu.VMEM((cpd, n_side), bf16),
            pltpu.VMEM((4, slots, d_model), bf16),
            dma((3 + 2 * extra,)), dma, dma, dma((3,)), dma((3,)),
        ] + gather_sems(n_seq // 2, 2) + [dma((n_seq - 1,)) for _ in range(4)]
        + [dma((3,)) for _ in range(8)],
        compiler_params=pltpu.CompilerParams(
            collective_id=number, has_side_effects=True, vmem_limit_bytes=60 * 1024 * 1024
        ),
        name="startup",
    )(tokens.reshape(2, here // 2, d_model), w_in, w_out, side, gains, route, cot)


class Fold:
    def __init__(self, arr, box, send, sems):
        self.arr, self.box, self.send, (self.s, self.r) = arr, box, send, sems
        self.mine, self.core, self.far, self.rest = dp_peers()

    def copy(self, k):
        src = [lambda: self.arr.at[self.core], lambda: self.arr.at[self.rest], lambda: self.send][k]()
        peer = self.far if k == 2 else self.core
        return remote(src, self.box.at[k], self.s.at[k], self.r.at[k], dp=peer)

    def start(self):
        self.copy(1).start()
        self.copy(0).start()

    def middle(self):
        self.copy(1).wait_recv()
        value = self.arr[self.far].astype(f32) + self.box[1].astype(f32)
        self.send[...] = value.astype(self.send.dtype)
        self.copy(2).start()

    def final(self):
        self.copy(0).wait_recv()
        self.copy(2).wait_recv()
        value = self.arr[self.mine].astype(f32) + self.box[0].astype(f32)
        return value + self.box[2].astype(f32)

    def done(self):
        for k in range(3):
            self.copy(k).wait_send()


class Finish:
    def __init__(
        self, n_seq, gwout, gwz, gw, pack, tok, gres, gains, ggmoe,
        gtok_out, gwout_out, pack_out, gwin_out, gain_out,
        gn, wsum, wbox, gst, gb1, gsum, gb2, o_box, o_send, w_box, w_send, z_box, z_send, p_box, p_send,
        lsem, *sems,
    ):
        self.line = Line(n_seq)
        self.tok, self.gres, self.gains, self.ggmoe = tok, gres, gains, ggmoe
        self.gtok_out, self.gwout_out, self.pack_out = gtok_out, gwout_out, pack_out
        self.gwin_out, self.gain_out = gwin_out, gain_out
        self.gn, self.wsum, self.wbox, self.gst, self.gb1 = gn, wsum, wbox, gst, gb1
        self.gsum, self.gb2, self.lsem = gsum, gb2, lsem
        self.sems, dsems = sems[8:14], sems[14:]

        def final(p, value):
            high = value.shape[0]
            gn[p * high : (p + 1) * high, :] = value

        self.stream = Made(self.line, sems[:8], final)
        self.f_w = Fold(gw, w_box, w_send, dsems[0:2])
        self.f_z = Fold(gwz, z_box, z_send, dsems[6:8])
        self.f_o = Fold(gwout, o_box, o_send, dsems[2:4])
        self.f_p = Fold(pack, p_box, p_send, dsems[4:6])

    def open(self):
        mine, core, far, rest = dp_peers()
        greet([(None, q) for q in all_peers(self.line.n_seq)], [core, far, rest])
        self.f_z.start()
        self.f_o.start()

    def early_middle(self):
        self.f_z.middle()
        self.f_o.middle()

    def block(self, half, q, r):
        a2s, a2r = self.sems[:2]
        return remote(self.wsum.at[half, q], self.wbox.at[half, self.line.me], a2s.at[half, r],
                      a2r.at[half, r], seq=q)

    def keep(self, half):
        me = self.line.me
        return pltpu.make_async_copy(self.wsum.at[half, me], self.wbox.at[half, me], self.lsem.at[half])

    def exchange(self, half, value):
        self.wsum[half] = value.astype(bf16)
        for r, q in enumerate(all_peers(self.line.n_seq)):
            self.block(half, q, r).start()
        self.keep(half).start()

    def early_final(self):
        self.exchange(1, self.f_z.final())
        self.gwout_out[...] = self.f_o.final()

    def close(self):
        line, f_w, f_o, f_p, stream = self.line, self.f_w, self.f_o, self.f_p, self.stream
        a2s, a2r, g1s, g1r, g2s, g2r = self.sems
        n_seq, me = line.n_seq, line.me
        peers = all_peers(n_seq)
        mine, core, far, rest = dp_peers()
        dps = [core, far, rest]
        f_p.start()
        stream.stage(0)
        f_w.middle()
        f_p.middle()
        for t in range(1, line.n - 1):
            stream.stage(t)
        self.exchange(0, f_w.final())
        copies = []
        self.pack_out[...] = f_p.final()
        if line.n > 2:
            stream.stage(line.n - 1)

        v = self.tok[...].astype(f32)
        r_ = lax.rsqrt(jnp.mean(v * v, axis=-1, keepdims=True) + eps)
        gy = self.gn[...]
        gst, gb1, gb2 = self.gst, self.gb1, self.gb2
        gst[0:1, :] = jnp.sum(gy * (v * r_), axis=0, keepdims=True)
        gst[1:2, :] = self.ggmoe[...]
        for k, peer in enumerate(dps):
            copy = remote(gst, gb1.at[k], g1s.at[k], g1r.at[k], dp=peer)
            copy.start()
            copies.append(copy)
        gyg = gy * self.gains[0:1, :]
        inner = jnp.mean(gyg * v, axis=-1, keepdims=True)
        self.gtok_out[...] = gyg * r_ - v * (r_ * r_ * r_ * inner) + self.gres[...]
        total = gst[...]
        for k in range(3):
            remote(gb1.at[k], gb1.at[k], g1s.at[k], g1r.at[k], dp=core).wait_recv()
            total = total + gb1[k]
        self.gsum[...] = total
        for r, q in enumerate(peers):
            copy = remote(self.gsum, gb2.at[r], g2s.at[r], g2r.at[r], seq=q)
            copy.start()
            copies.append(copy)

        for half in range(2):
            self.keep(half).wait()
            for r, q in enumerate(peers):
                here = self.wbox.at[half, lax.rem(me + n_seq - 1 - r, n_seq)]
                remote(here, here, a2s.at[half, r], a2r.at[half, r], seq=q).wait_recv()
        wide = self.gwin_out.shape[1]
        cpd = wide // (2 * 4 * n_seq)
        for q in range(n_seq):
            for half in range(2):
                block = self.wbox[half, q].astype(f32)
                for p in range(4):
                    at = (half * 4 * n_seq + p * n_seq + q) * cpd
                    self.gwin_out[:, at : at + cpd] = block[:, p * cpd : (p + 1) * cpd]
        for r, q in enumerate(peers):
            remote(gb2.at[r], gb2.at[r], g2s.at[r], g2r.at[r], seq=q).wait_recv()
            total = total + gb2[r]
        self.gain_out[...] = total
        stream.finish()
        for fold in (f_w, self.f_z, f_o, f_p):
            fold.done()
        for half in range(2):
            for r, q in enumerate(peers):
                self.block(half, q, r).wait_send()
        for copy in copies:
            copy.wait_send()


def finish_scratch(n_seq, here, d_model, high, wide, cpd, n_side):
    dma = pltpu.SemaphoreType.DMA
    mem = pltpu.VMEM
    many = dma((n_seq - 1,))
    return [
        mem((here, d_model), f32), mem((2, n_seq, high, wide), bf16), mem((2, n_seq, high, wide), bf16),
        mem((2, d_model), f32), mem((3, 2, d_model), f32), mem((2, d_model), f32),
        mem((n_seq - 1, 2, d_model), f32),
        mem((3, cpd, d_model), bf16), mem((cpd, d_model), bf16),
        mem((3, n_seq, high, wide), bf16), mem((n_seq, high, wide), bf16),
        mem((3, n_seq, high, wide), bf16), mem((n_seq, high, wide), bf16),
        mem((3, cpd, n_side), f32), mem((cpd, n_side), f32), dma((2,)),
    ] + made_scratch(n_seq // 2, 2, here // 2, d_model) + [
        dma((2, n_seq - 1)), dma((2, n_seq - 1)), dma((3,)), dma((3,)), many, many
    ] + [dma((3,)) for _ in range(8)]


def on_device(
    tokens, route, cotangent, gain_mix, w_in, conv_w, w_x, w_dt, dt_bias, a_log, d_skip, w_out,
    gain_moe, w_up, w_down,
):
    n_seq, n_dp = lax.axis_size("seq"), lax.axis_size("dp")
    here, d_model = tokens.shape
    cpd = conv_w.shape[0]
    chans = cpd * n_dp
    cp = up128(chans)
    rank = w_dt.shape[1]
    n_small = w_x.shape[1]
    sp = up128(n_small)
    tall = here * n_seq
    rows_in = w_in.shape[0]
    experts, slots = n_dp, 40

    gap = jnp.zeros((cpd, 128), bf16)
    side = jnp.concatenate(
        [w_x[:, :rank], gap[:, rank:B_AT], w_x[:, rank:], gap[:, C_AT + NS :], w_dt, gap[:, rank:], conv_w, gap[:, 4:8], dt_bias[:, None],
         d_skip[:, None], gap[:, 10:16], a_log, gap[:, 32:]], axis=1,
    )
    gains_in = jnp.pad(jnp.stack([gain_mix, gain_moe]).astype(f32), ((0, 6), (0, 128 - gain_mix.shape[0])))
    xg, w_all, wout_all, side_all, gain_all, cot_own, pick = start_call(
        tokens, w_in, w_out, side, gains_in, route, cotangent, slots, n_seq, cp, 0
    )
    toks = xg.reshape(tall, d_model)
    w_mine = w_all.reshape(n_dp * n_seq * rows_in, 2 * cp)
    wout_m = wout_all.reshape(-1, d_model)
    side_m = side_all.reshape(-1, 384)
    gains = gain_all[:, :, :2, : gain_mix.shape[0]].transpose(2, 1, 0, 3).reshape(2, d_model)
    wout_spec = (((cp, d_model), 0),)
    wx_spec, wdt_spec, misc_spec = [(((cp, 128), k),) for k in range(3)]

    row_values = tokens.astype(f32)
    tb = 128
    steps = tall // tb
    sds = jax.ShapeDtypeStruct
    wide = sds((tall, cp), f32)
    vec = pltpu.VMEM((tb, cp), f32)
    turned_misc = pltpu.VMEM((128, cp), f32)
    by_state = pltpu.VMEM((NS, cp), f32)
    x, z, conv, normed, small, grad_slots = chunked(
        partial(in_kernel, n_seq, steps), steps, False,
        [(toks, tb), (gains, 0), (w_mine, 0), (side_m, wx_spec), (side_m, misc_spec),
         (cot_own, None)],
        [(wide, tb), (wide, tb), (wide, tb), (sds((tall, d_model), bf16), tb),
         (sds((n_seq, tb, sp), bf16), None), (sds((n_seq, n_dp, slots, d_model), bf16), None)],
        [pltpu.VMEM((tb + 8, cp), f32), turned_misc, pltpu.SemaphoreType.DMA]
        + gather_sems(n_seq // 2, n_dp) + sum_scratch(n_seq, tb, sp), "mix_in", 1,
    )
    small = small.reshape(tall, sp)
    dtp, delta, u_all, hs, ssm, gated, mixer_out, grad_slots = chunked(
        partial(scan_kernel, n_seq, steps), steps, False,
        [(small, tb), (side_m, wdt_spec), (side_m, misc_spec), (conv, tb), (z, tb),
         (wout_m, wout_spec), (cot_own, None), (grad_slots, None)],
        [(wide, tb), (wide, tb), (wide, tb), (sds((tall, NS, cp), f32), tb), (wide, tb),
         (sds((tall, cp), bf16), tb), (sds((here, d_model), f32), 0),
         (sds((n_seq, n_dp, slots, d_model), bf16), None)],
        [vec, by_state, turned_misc, by_state, pltpu.VMEM((2 * NS, tb), f32)]
        + gather_sems(n_seq // 2, n_dp) + made_scratch(n_seq // 2, 2, here // 2, d_model),
        "scan_forward", 3, {7: 7},
    )
    grad_slots = grad_slots.reshape(n_seq * n_dp * slots, d_model)
    resid = row_values + mixer_out

    normed2, norm2_pullback = jax.vjp(rms_norm, resid, gains[1])
    moe_in = normed2.astype(bf16)
    def dispatch(values, number):
        send = mm(pick, values, TN).astype(bf16).reshape(n_dp, slots, d_model)
        return dispatch_call(send, n_seq, number).reshape(n_seq * n_dp * slots, d_model)

    def returned(sums):
        return mm(pick, sums.reshape(n_dp * slots, d_model))

    shape4 = (n_seq, n_dp, slots, d_model)
    up, down = w_up[0], w_down[0]
    grad_hidden = mm(grad_slots, down, NT)
    slot_rows = dispatch(moe_in, 4)
    pre_act = mm(slot_rows, up, NT)
    hidden_f, gelu_pullback = jax.vjp(partial(jax.nn.gelu, approximate=False), pre_act)
    hidden = hidden_f.astype(bf16)
    grad_pre = gelu_pullback(grad_hidden)[0].astype(bf16)
    grad_moe_in = returned(collect_call(mm(grad_pre, up).astype(bf16).reshape(shape4), n_seq, 5))
    expert_terms = mm(hidden, down).astype(bf16).reshape(shape4)
    grad_down = mm(hidden, grad_slots, TN)
    grad_up = mm(grad_pre, slot_rows, TN)

    grad_resid, grad_gmoe = norm2_pullback(grad_moe_in)
    grad_resid = grad_resid + cotangent.astype(f32)
    gml = seq_gather(grad_resid.astype(bf16), n_seq, 2, 7)
    gu, gz, gwout, gwdt, gmisc, gwz, expert_out, gsmall = chunked(
        partial(back_kernel, n_seq, steps), steps, True,
        [(gml, tb), (wout_m, wout_spec), (gated, tb), (u_all, tb), (z, tb), (ssm, tb), (delta, tb), (dtp, tb),
         (hs, tb), (hs, -tb), (small, tb), (side_m, wdt_spec), (side_m, misc_spec), (expert_terms, 0),
         (normed, tb)],
        [(wide, tb), (sds((tall, cp), bf16), tb), (sds((n_dp, cpd, d_model), bf16), 0),
         (sds((cp, sp), f32), 0), (sds((32, cp), f32), 0), (sds((n_dp, n_seq, rows_in, cp), bf16), 0),
         (sds((n_dp, slots, d_model), bf16), None),
         (sds((n_seq, tb, sp), bf16), None)],
        [vec] * 4 + [by_state, turned_misc, by_state, pltpu.VMEM((2 * NS, tb), f32),
                     pltpu.VMEM((tb, NS, cp), bf16), pltpu.VMEM((cp, d_model), f32), by_state,
                     pltpu.VMEM((d_model, cp), f32)]
        + collect_scratch(n_seq, n_dp, slots, d_model) + sum_scratch(n_seq, tb, sp),
        "scan_backward", 6,
    )
    gsmall = gsmall.reshape(tall, sp)
    result = (resid + returned(expert_out)).astype(bf16)
    grad_tokens, grad_wout, gpack, grad_win, ggains = chunked(
        partial(out_kernel, n_seq, steps), steps, True,
        [(gsmall, tb), (side_m, wx_spec), (side_m, misc_spec), (conv, tb), (x, tb), (gu, tb), (gz, tb),
         (normed, tb), (w_mine, 0), (gwdt, 0), (gmisc, 0), (gwout, 0), (gwz, 0), (tokens, 0), (grad_resid, 0),
         (gains, 0), (grad_gmoe[None], 0)],
        [(sds((here, d_model), f32), 0), (sds((cpd, d_model), f32), 0), (sds((cpd, 384), f32), 0),
         (sds((rows_in, 2 * 4 * n_seq * cpd), f32), 0), (sds((2, d_model), f32), 0)],
        [pltpu.VMEM((tb + 8, cp), f32), turned_misc, pltpu.VMEM((cp, sp), f32),
         pltpu.VMEM((d_model, cp), f32), turned_misc,
         pltpu.VMEM((n_dp, n_seq, rows_in, cp), bf16), pltpu.VMEM((n_dp, cpd, 384), f32)]
        + finish_scratch(n_seq, here, d_model, rows_in, cp, cpd, 384), "finish", 9,
    )
    own = gain_mix.shape[0]
    ggains = lax.dynamic_slice(
        ggains, (0, (lax.axis_index("dp") * n_seq + lax.axis_index("seq")) * own), (2, own)
    )
    return (
        result, grad_tokens, ggains[0], grad_win, gpack[:, 256:260],
        jnp.concatenate([gpack[:, :rank], gpack[:, B_AT : C_AT + NS]], axis=1),
        gpack[:, 128 : 128 + rank], gpack[:, 264], gpack[:, 272 : 272 + NS], gpack[:, 265],
        grad_wout, ggains[1], grad_up[None], grad_down[None],
    )


def solution(mesh):
    row2, row1 = P(("dp", "seq"), None), P(("dp", "seq"))
    mats = P("dp", "seq", None)
    return jax.shard_map(
        on_device,
        mesh=mesh,
        in_specs=(
            row2, row2, row2, row1, row2, row2, row2, row2, row1, row2, row1, row2, row1, mats, mats
        ),
        out_specs=(
            row2, row2, row1, row2, row2, row2, row2, row1, row2, row1, row2, row1, mats, mats
        ),
        check_vma=False,
    )
```
